8 devices in a mesh: dp: 1 (over z), tp: 8 (over y, x, core).
Axes of the slice: x: 2, y: 2, z: 1, core: 2. Of those that a mesh axis runs over, the one named last changes fastest.
Arguments:
- resid_in: bfloat16 [128, 8192], P('dp')
- positions: int32 [128], P('dp')
- k_cache: bfloat16 [128, 128, 8, 128], P('dp', None, 'tp')
- v_cache: bfloat16 [128, 128, 8, 128], P('dp', None, 'tp')
- gain_attn: bfloat16 [8192], replicated
- w_query: bfloat16 [8192, 8192], P(None, 'tp')
- w_key: bfloat16 [8192, 1024], P(None, 'tp')
- w_value: bfloat16 [8192, 1024], P(None, 'tp')
- w_out: bfloat16 [8192, 8192], P('tp')
- gain_mlp: bfloat16 [8192], replicated
- w_gate: bfloat16 [8192, 22016], P(None, 'tp')
- w_up: bfloat16 [8192, 22016], P(None, 'tp')
- w_down: bfloat16 [22016, 8192], P('tp')
Outputs:
- output 1: bfloat16 [128, 8192], P('dp')
- output 2: bfloat16 [128, 128, 8, 128], P('dp', None, 'tp')
- output 3: bfloat16 [128, 128, 8, 128], P('dp', None, 'tp')
All inputs are finite; a program needn't handle non-finite values.
Results may differ from the reference program's by a relative error of at most 0.010786.
Values sent between devices are 32-bit elements.
A program may use at most 1 GiB of HBM per device.

```python
import math
import jax
import jax.numpy as jnp
from jax import lax

BATCH_PART = 128
CACHE_LEN = 128
MODEL_DIM = 8192
Q_HEADS = 64
KV_HEADS = 8
HEAD_DIM = 128
FFN_DIM = 22016

EPS = 1e-5
ROPE_THETA = 500000.0
ROPE_FACTOR = 8.0
LOW_FACTOR = 1.0
HIGH_FACTOR = 4.0
ORIG_CTX = 8192.0


def setup_inputs(seed: int = 0, part: int = 0) -> dict:
    part_keys = jax.random.split(jax.random.fold_in(jax.random.key(seed), part), 6)
    weight_keys = jax.random.split(jax.random.key(seed + 1), 11)
    log_len = int(math.log2(CACHE_LEN))
    dim_scale = 1.0 / math.sqrt(MODEL_DIM)
    out_scale = 1.0 / math.sqrt(Q_HEADS * HEAD_DIM)
    ffn_scale = 1.0 / math.sqrt(FFN_DIM)
    q_width = Q_HEADS * HEAD_DIM
    kv_width = KV_HEADS * HEAD_DIM
    resid_in = jax.random.normal(part_keys[0], (BATCH_PART, MODEL_DIM), jnp.float32)
    exponent = jax.random.randint(part_keys[1], (BATCH_PART,), 0, log_len + 1, dtype=jnp.int32)
    upper_bound = jnp.left_shift(jnp.ones((BATCH_PART,), jnp.int32), exponent)
    positions = jax.random.randint(part_keys[2], (BATCH_PART,), 0, upper_bound, dtype=jnp.int32)
    positions = positions.at[0].set(CACHE_LEN - 1).at[1].set(0)
    cache_shape = (BATCH_PART, CACHE_LEN, KV_HEADS, HEAD_DIM)
    k_cache = jax.random.normal(part_keys[3], cache_shape, jnp.float32)
    v_mean = 0.7 * jax.random.normal(part_keys[4], (BATCH_PART, 1, KV_HEADS, HEAD_DIM), jnp.float32)
    v_cache = v_mean + jax.random.normal(part_keys[5], cache_shape, jnp.float32)
    gain_attn = 1.0 + 0.3 * jax.random.normal(weight_keys[0], (MODEL_DIM,), jnp.float32)
    w_query = jax.random.normal(weight_keys[1], (MODEL_DIM, q_width), jnp.float32) * dim_scale
    w_key = jax.random.normal(weight_keys[2], (MODEL_DIM, kv_width), jnp.float32) * dim_scale
    w_value = jax.random.normal(weight_keys[3], (MODEL_DIM, kv_width), jnp.float32) * dim_scale
    w_out = jax.random.normal(weight_keys[4], (q_width, MODEL_DIM), jnp.float32) * out_scale
    gain_mlp = 1.0 + 0.3 * jax.random.normal(weight_keys[5], (MODEL_DIM,), jnp.float32)
    w_gate = jax.random.normal(weight_keys[6], (MODEL_DIM, FFN_DIM), jnp.float32) * dim_scale
    w_up = jax.random.normal(weight_keys[7], (MODEL_DIM, FFN_DIM), jnp.float32) * dim_scale
    w_down = jax.random.normal(weight_keys[8], (FFN_DIM, MODEL_DIM), jnp.float32) * ffn_scale
    return dict(resid_in=resid_in.astype(jnp.bfloat16), positions=positions,
                k_cache=k_cache.astype(jnp.bfloat16), v_cache=v_cache.astype(jnp.bfloat16),
                gain_attn=gain_attn.astype(jnp.bfloat16), w_query=w_query.astype(jnp.bfloat16),
                w_key=w_key.astype(jnp.bfloat16), w_value=w_value.astype(jnp.bfloat16),
                w_out=w_out.astype(jnp.bfloat16), gain_mlp=gain_mlp.astype(jnp.bfloat16),
                w_gate=w_gate.astype(jnp.bfloat16), w_up=w_up.astype(jnp.bfloat16),
                w_down=w_down.astype(jnp.bfloat16))


def rms_norm(rows_in, gain):
    rows_f = rows_in.astype(jnp.float32)
    mean_sq = jnp.mean(rows_f * rows_f, axis=-1, keepdims=True)
    return (rows_f * lax.rsqrt(mean_sq + EPS) * gain.astype(jnp.float32)).astype(jnp.bfloat16)


def rope_tables(positions, head_dim):
    half_dim = head_dim // 2
    exponents = jnp.arange(half_dim, dtype=jnp.float32) * (2.0 / head_dim)
    inv_freq = 1.0 / jnp.power(ROPE_THETA, exponents)
    wavelen = (2.0 * math.pi) / inv_freq
    smooth = (ORIG_CTX / wavelen - LOW_FACTOR) / (HIGH_FACTOR - LOW_FACTOR)
    blended = (1.0 - smooth) * inv_freq / ROPE_FACTOR + smooth * inv_freq
    inv_freq = jnp.where(wavelen < ORIG_CTX / HIGH_FACTOR, inv_freq,
                         jnp.where(wavelen > ORIG_CTX / LOW_FACTOR, inv_freq / ROPE_FACTOR, blended))
    angles = positions.astype(jnp.float32)[:, None] * inv_freq[None, :]
    return jnp.cos(angles), jnp.sin(angles)


def apply_rope(vectors, cos_t, sin_t):
    half_dim = vectors.shape[-1] // 2
    lower_half = vectors[..., :half_dim]
    upper_half = vectors[..., half_dim:]
    cos_b = cos_t[:, None, :]
    sin_b = sin_t[:, None, :]
    return jnp.concatenate([lower_half * cos_b - upper_half * sin_b,
                            upper_half * cos_b + lower_half * sin_b], axis=-1)


def reference(resid_in, positions, k_cache, v_cache, gain_attn, w_query, w_key, w_value,
              w_out, gain_mlp, w_gate, w_up, w_down):
    group_size = Q_HEADS // KV_HEADS
    n_seqs = resid_in.shape[0]
    normed = rms_norm(resid_in, gain_attn)
    queries = jnp.dot(normed, w_query, preferred_element_type=jnp.float32).astype(jnp.bfloat16)
    key_new = jnp.dot(normed, w_key, preferred_element_type=jnp.float32).astype(jnp.bfloat16)
    value_new = jnp.dot(normed, w_value, preferred_element_type=jnp.float32).astype(jnp.bfloat16)
    cos_t, sin_t = rope_tables(positions, HEAD_DIM)
    queries = apply_rope(queries.reshape(n_seqs, Q_HEADS, HEAD_DIM).astype(jnp.float32), cos_t, sin_t)
    queries = queries.astype(jnp.bfloat16)
    key_new = apply_rope(key_new.reshape(n_seqs, KV_HEADS, HEAD_DIM).astype(jnp.float32), cos_t, sin_t)
    key_new = key_new.astype(jnp.bfloat16)
    value_new = value_new.reshape(n_seqs, KV_HEADS, HEAD_DIM)
    slot_hit = (jnp.arange(CACHE_LEN)[None, :] == positions[:, None])[:, :, None, None]
    k_full = jnp.where(slot_hit, key_new[:, None], k_cache)
    v_full = jnp.where(slot_hit, value_new[:, None], v_cache)
    scale = 1.0 / math.sqrt(HEAD_DIM)

    def one_seq(seq_items):
        q_seq, k_seq, v_seq, pos_seq = seq_items
        q_grp = q_seq.reshape(KV_HEADS, group_size, HEAD_DIM).astype(jnp.float32)
        scores = jnp.einsum('kgd,skd->kgs', q_grp, k_seq.astype(jnp.float32)) * scale
        valid = jnp.arange(CACHE_LEN) <= pos_seq
        scores = jnp.where(valid[None, None, :], scores, -jnp.inf)
        attn_prob = jax.nn.softmax(scores, axis=-1).astype(jnp.bfloat16)
        attn_seq = jnp.einsum('kgs,skd->kgd', attn_prob.astype(jnp.float32), v_seq.astype(jnp.float32))
        return attn_seq.astype(jnp.bfloat16).reshape(Q_HEADS * HEAD_DIM)

    attn_out = lax.map(one_seq, (queries, k_full, v_full, positions))
    y_full = jnp.dot(attn_out, w_out, preferred_element_type=jnp.float32)
    resid_mid = (resid_in.astype(jnp.float32) + y_full).astype(jnp.bfloat16)
    normed_mlp = rms_norm(resid_mid, gain_mlp)
    gate_proj = jnp.dot(normed_mlp, w_gate, preferred_element_type=jnp.float32).astype(jnp.bfloat16)
    up_proj = jnp.dot(normed_mlp, w_up, preferred_element_type=jnp.float32).astype(jnp.bfloat16)
    hidden = (jax.nn.silu(gate_proj.astype(jnp.float32)) * up_proj.astype(jnp.float32)).astype(jnp.bfloat16)
    z_full = jnp.dot(hidden, w_down, preferred_element_type=jnp.float32)
    resid_out = (resid_mid.astype(jnp.float32) + z_full).astype(jnp.bfloat16)
    return resid_out, k_full, v_full
```

```python
import math
import jax
import jax.numpy as jnp
from jax import lax
from jax.experimental import pallas as pl
from jax.experimental.pallas import tpu as pltpu
from jax.sharding import PartitionSpec as P

EPS = 1e-5
ROPE_THETA = 500000.0
ROPE_FACTOR = 8.0
LOW_FACTOR = 1.0
HIGH_FACTOR = 4.0
ORIG_CTX = 8192.0


def rms_norm(rows_in, gain):
    rows_f = rows_in.astype(jnp.float32)
    mean_sq = jnp.mean(rows_f * rows_f, axis=-1, keepdims=True)
    return (rows_f * lax.rsqrt(mean_sq + EPS) * gain.astype(jnp.float32)).astype(jnp.bfloat16)


def rope_tables(positions, head_dim):
    half_dim = head_dim // 2
    exponents = jnp.arange(half_dim, dtype=jnp.float32) * (2.0 / head_dim)
    inv_freq = 1.0 / jnp.power(ROPE_THETA, exponents)
    wavelen = (2.0 * math.pi) / inv_freq
    smooth = (ORIG_CTX / wavelen - LOW_FACTOR) / (HIGH_FACTOR - LOW_FACTOR)
    blended = (1.0 - smooth) * inv_freq / ROPE_FACTOR + smooth * inv_freq
    inv_freq = jnp.where(wavelen < ORIG_CTX / HIGH_FACTOR, inv_freq,
                         jnp.where(wavelen > ORIG_CTX / LOW_FACTOR, inv_freq / ROPE_FACTOR, blended))
    angles = positions.astype(jnp.float32)[:, None] * inv_freq[None, :]
    return jnp.cos(angles), jnp.sin(angles)


def apply_rope(vectors, cos_t, sin_t):
    half_dim = vectors.shape[-1] // 2
    lower_half = vectors[..., :half_dim]
    upper_half = vectors[..., half_dim:]
    cos_b = cos_t[:, None, :]
    sin_b = sin_t[:, None, :]
    return jnp.concatenate([lower_half * cos_b - upper_half * sin_b,
                            upper_half * cos_b + lower_half * sin_b], axis=-1)


def attention_block(resid_in, positions, k_cache, v_cache, gain_attn, w_query, w_key, w_value):
    n_seqs = resid_in.shape[0]
    cache_len = k_cache.shape[1]
    kv_heads = k_cache.shape[2]
    head_dim = k_cache.shape[3]
    group_size = w_query.shape[1] // (kv_heads * head_dim)
    normed = rms_norm(resid_in, gain_attn)
    queries = jnp.dot(normed, w_query, preferred_element_type=jnp.float32).astype(jnp.bfloat16)
    key_new = jnp.dot(normed, w_key, preferred_element_type=jnp.float32).astype(jnp.bfloat16)
    value_new = jnp.dot(normed, w_value, preferred_element_type=jnp.float32).astype(jnp.bfloat16)
    cos_t, sin_t = rope_tables(positions, head_dim)
    queries = apply_rope(queries.reshape(n_seqs, kv_heads * group_size, head_dim).astype(jnp.float32), cos_t, sin_t)
    queries = queries.astype(jnp.bfloat16).reshape(n_seqs, kv_heads, group_size, head_dim)
    key_new = apply_rope(key_new.reshape(n_seqs, kv_heads, head_dim).astype(jnp.float32), cos_t, sin_t)
    key_new = key_new.astype(jnp.bfloat16)
    value_new = value_new.reshape(n_seqs, kv_heads, head_dim)
    slot_iota = lax.broadcasted_iota(jnp.int32, (n_seqs, cache_len), 1)
    slot_hit = (slot_iota == positions[:, None])[:, :, None, None]
    k_full = jnp.where(slot_hit, key_new[:, None], k_cache)
    v_full = jnp.where(slot_hit, value_new[:, None], v_cache)
    scores = jnp.einsum('bkgd,bskd->bkgs', queries, k_full, preferred_element_type=jnp.float32)
    scores = scores * (1.0 / math.sqrt(head_dim))
    valid = (slot_iota <= positions[:, None])[:, None, None, :]
    scores = jnp.where(valid, scores, -jnp.inf)
    attn_prob = jax.nn.softmax(scores, axis=-1).astype(jnp.bfloat16)
    attn_out = jnp.einsum('bkgs,bskd->bkgd', attn_prob, v_full, preferred_element_type=jnp.float32)
    attn_out = attn_out.astype(jnp.bfloat16).reshape(n_seqs, kv_heads * group_size * head_dim)
    return attn_out, k_full, v_full


N_CHUNK = 16
N_SLOT = 15
MESH = pl.DeviceIdType.MESH


def tail_kernel(attn_ref, resid_hbm, gain_ref, w_out_hbm, gate_t_hbm, up_t_hbm, w_down_hbm, out_ref,
                part, from_core, from_x1, from_y1, from_x2, from_y2, gathered, mid, sq_sum, resid_own,
                gate_acc, up_acc, hidden, ring,
                resid_sem, out_sem, ring_sem, rs_send, rs_recv, ag_send, ag_recv):
    n_chunk, chunk = N_CHUNK, part.shape[-1]
    half = chunk // 2
    rows = mid.shape[1]
    me = lax.axis_index('tp')
    k = me % 2
    x = (me // 2) % 2
    y = me // 4
    nk, nx, ny = 1 - k, 1 - x, 1 - y
    core_nbr = {'tp': me + 1 - 2 * k}
    x_nbr = {'tp': me + 2 - 4 * x}
    y_nbr = {'tp': me + 4 - 8 * y}

    def cols(c):
        return pl.ds(pl.multiple_of(c * chunk, chunk), chunk)

    depth_out = w_out_hbm.shape[0]
    first_mlp = n_chunk // 2
    first_down = first_mlp + 2 * n_chunk

    def out_slot(c):
        return c // 2, pl.ds(pl.multiple_of((c % 2) * depth_out, depth_out), depth_out)

    def out_copy(c):
        slot, span = out_slot(c)
        return pltpu.make_async_copy(w_out_hbm.at[:, cols(c)], ring.at[slot, span], out_sem.at[c])

    def ring_copy(src, c, j):
        slot = j % N_SLOT
        return pltpu.make_async_copy(src.at[:, cols(c)], ring.at[slot], ring_sem.at[slot])

    def gate_copy(c):
        return ring_copy(gate_t_hbm, c, first_mlp + 2 * c)

    def up_copy(c):
        return ring_copy(up_t_hbm, c, first_mlp + 2 * c + 1)

    def down_copy(c):
        return ring_copy(w_down_hbm, c, first_down + c)

    def start_load(j):
        m = j - first_mlp

        @pl.when(j < first_down)
        def _():
            @pl.when(m % 2 == 0)
            def _():
                gate_copy(m // 2).start()

            @pl.when(m % 2 == 1)
            def _():
                up_copy(m // 2).start()

        @pl.when(jnp.logical_and(j >= first_down, j < first_down + n_chunk))
        def _():
            down_copy(j - first_down).start()

    row0 = pl.multiple_of(64 * k + 32 * x + 16 * y, 16)
    resid_copy = pltpu.make_async_copy(resid_hbm.at[pl.ds(row0, rows)], resid_own, resid_sem)
    for c in range(2):
        out_copy(c).start()
    resid_copy.start()
    for c in range(2, n_chunk):
        out_copy(c).start()
    for j in range(first_mlp, N_SLOT):
        (up_copy if (j - first_mlp) % 2 else gate_copy)((j - first_mlp) // 2).start()

    barrier = pltpu.get_barrier_semaphore()
    for nbr in (core_nbr, x_nbr, y_nbr):
        pl.semaphore_signal(barrier, inc=1, device_id=nbr, device_id_type=MESH)

    def remote(src, dst, sems, ch, c, nbr):
        return pltpu.make_async_remote_copy(src_ref=src, dst_ref=dst, send_sem=sems[0].at[ch, c],
                                            recv_sem=sems[1].at[ch, c], device_id=nbr, device_id_type=MESH)

    rs = (rs_send, rs_recv)
    ag = (ag_send, ag_recv)
    left, right = pl.ds(0, half), pl.ds(half, half)

    def rs_core(c):
        return remote(part.at[c, nk], from_core.at[c], rs, 0, c, core_nbr)

    def rs_x1(c):
        return remote(part.at[c, k, nx, :, :, left], from_x1.at[c], rs, 1, c, x_nbr)

    def rs_y1(c):
        return remote(part.at[c, k, :, ny, :, right], from_y1.at[c], rs, 2, c, y_nbr)

    def rs_y2(c):
        return remote(part.at[c, k, x, ny, :, left], from_y2.at[c], rs, 3, c, y_nbr)

    def rs_x2(c):
        return remote(part.at[c, k, nx, y, :, right], from_x2.at[c], rs, 4, c, x_nbr)

    def ag_x(c):
        blk = gathered.at[c, k, x, y]
        return remote(blk, blk, ag, 0, c, x_nbr)

    def ag_y(c):
        blk = gathered.at[c, k, x, y]
        return remote(blk, blk, ag, 1, c, y_nbr)

    def ag_fwd_y(c):
        blk = gathered.at[c, k, nx, y, :, right]
        return remote(blk, blk, ag, 2, c, y_nbr)

    def ag_fwd_x(c):
        blk = gathered.at[c, k, x, ny, :, left]
        return remote(blk, blk, ag, 3, c, x_nbr)

    def ag_core(c):
        blk = gathered.at[c, k]
        return remote(blk, blk, ag, 4, c, core_nbr)

    def stage(s, lag, fn):
        c = s - lag

        @pl.when(jnp.logical_and(c >= 0, c < n_chunk))
        def _():
            fn(c)

    def rs_stage1(c):
        rs_core(c).wait_recv()
        part[c, k] = part[c, k] + from_core[c]
        rs_x1(c).start()
        rs_y1(c).start()

    def rs_stage2(c):
        rs_x1(c).wait_recv()
        part[c, k, x, :, :, left] = part[c, k, x, :, :, left] + from_x1[c]
        rs_y2(c).start()
        rs_y1(c).wait_recv()
        part[c, k, :, y, :, right] = part[c, k, :, y, :, right] + from_y1[c]
        rs_x2(c).start()

    def rs_stage3(c):
        rs_y2(c).wait_recv()
        rs_x2(c).wait_recv()
        total = jnp.concatenate([part[c, k, x, y, :, left] + from_y2[c],
                                 part[c, k, x, y, :, right] + from_x2[c]], axis=-1)
        for copy in (rs_core, rs_x1, rs_y1, rs_y2, rs_x2):
            copy(c).wait_send()
        return total

    def ag_stage1(c):
        ag_x(c).wait_recv()
        ag_fwd_y(c).start()
        ag_y(c).wait_recv()
        ag_fwd_x(c).start()

    def ag_stage2(c):
        ag_fwd_x(c).wait_recv()
        ag_fwd_y(c).wait_recv()
        ag_core(c).start()

    def ag_stage3(c):
        ag_core(c).wait_recv()
        block = gathered[c].reshape(8 * rows, chunk)
        for copy in (ag_x, ag_y, ag_fwd_x, ag_fwd_y, ag_core):
            copy(c).wait_send()
        return block

    pl.semaphore_wait(barrier, 3)
    sq_sum[...] = jnp.zeros_like(sq_sum)
    resid_copy.wait()

    def proj(c):
        out_copy(c).wait()
        slot, span = out_slot(c)
        res = jnp.dot(attn_ref[...], ring[slot, span], preferred_element_type=jnp.float32)
        part[c] = res.reshape(part.shape[1:])
        rs_core(c).start()

        @pl.when(c % 2 == 1)
        def _():
            start_load(c // 2 + N_SLOT)

    def finish_mid(c):
        total = rs_stage3(c)
        x1 = (resid_own[:, cols(c)].astype(jnp.float32) + total).astype(jnp.bfloat16).astype(jnp.float32)
        mid[c] = x1
        sq_sum[...] += x1 * x1

    def rs_body(s, carry):
        stage(s, RS_LAG[0], rs_stage1)
        stage(s, RS_LAG[1], rs_stage2)
        stage(s, RS_LAG[2], finish_mid)
        stage(s, 0, proj)
        return carry

    lax.fori_loop(0, n_chunk + RS_LAG[2], rs_body, 0)

    mean_sq = jnp.sum(sq_sum[...], axis=-1, keepdims=True) * (1.0 / (n_chunk * chunk))
    scale = lax.rsqrt(mean_sq + EPS)
    gate_acc[...] = jnp.zeros_like(gate_acc)
    up_acc[...] = jnp.zeros_like(up_acc)

    def send_normed(c):
        normed = (mid[c] * scale * gain_ref[:, cols(c)].astype(jnp.float32)).astype(jnp.bfloat16)
        gathered[c, k, x, y] = normed.astype(jnp.float32)
        ag_x(c).start()
        ag_y(c).start()

    def gate_up(c):
        block = ag_stage3(c).astype(jnp.bfloat16)
        for copy, acc, j in ((gate_copy, gate_acc, first_mlp + 2 * c), (up_copy, up_acc, first_mlp + 2 * c + 1)):
            copy(c).wait()
            acc[...] += lax.dot_general(block, ring[j % N_SLOT], (((1,), (1,)), ((), ())),
                                        preferred_element_type=jnp.float32)
            start_load(j + N_SLOT)

    def ag_body(s, carry):
        stage(s, AG_LAG[0], ag_stage1)
        stage(s, AG_LAG[1], ag_stage2)
        stage(s, 0, send_normed)
        stage(s, AG_LAG[2], gate_up)
        return carry

    lax.fori_loop(0, n_chunk + AG_LAG[2], ag_body, 0)

    gate = gate_acc[...].astype(jnp.bfloat16).astype(jnp.float32)
    up = up_acc[...].astype(jnp.bfloat16).astype(jnp.float32)
    hidden[...] = (jax.nn.silu(gate) * up).astype(jnp.bfloat16)

    def down(c):
        down_copy(c).wait()
        j = first_down + c
        res = jnp.dot(hidden[...], ring[j % N_SLOT], preferred_element_type=jnp.float32)
        part[c] = res.reshape(part.shape[1:])
        rs_core(c).start()
        start_load(j + N_SLOT)

    def finish_out(c):
        total = rs_stage3(c)
        gathered[c, k, x, y] = (mid[c] + total).astype(jnp.bfloat16).astype(jnp.float32)
        ag_x(c).start()
        ag_y(c).start()

    def store_out(c):
        out_ref[:, cols(c)] = ag_stage3(c).astype(jnp.bfloat16)

    base = RS_LAG[2]

    def down_body(s, carry):
        stage(s, RS_LAG[0], rs_stage1)
        stage(s, RS_LAG[1], rs_stage2)
        stage(s, base, finish_out)
        stage(s, base + AG_LAG[0], ag_stage1)
        stage(s, base + AG_LAG[1], ag_stage2)
        stage(s, 0, down)
        stage(s, base + AG_LAG[2], store_out)
        return carry

    lax.fori_loop(0, n_chunk + base + AG_LAG[2], down_body, 0)


RS_LAG = (1, 4, 7)
AG_LAG = (3, 6, 8)


def layer_tail(attn_out, resid_in, gain_mlp, w_out, w_gate, w_up, w_down):
    n_rows, width = resid_in.shape
    ffn = w_gate.shape[1]
    chunk = width // N_CHUNK
    half = chunk // 2
    rows = n_rows // 8
    f32, bf16 = jnp.float32, jnp.bfloat16
    vmem = pl.BlockSpec(memory_space=pltpu.VMEM)
    hbm = pl.BlockSpec(memory_space=pl.ANY)
    dma = pltpu.SemaphoreType.DMA
    return pl.pallas_call(
        tail_kernel,
        out_shape=jax.ShapeDtypeStruct((n_rows, width), bf16),
        in_specs=[vmem, hbm, vmem, hbm, hbm, hbm, hbm],
        out_specs=vmem,
        scratch_shapes=[
            pltpu.VMEM((N_CHUNK, 2, 2, 2, rows, chunk), f32),
            pltpu.VMEM((N_CHUNK, 2, 2, rows, chunk), f32),
            pltpu.VMEM((N_CHUNK, 2, rows, half), f32),
            pltpu.VMEM((N_CHUNK, 2, rows, half), f32),
            pltpu.VMEM((N_CHUNK, rows, half), f32),
            pltpu.VMEM((N_CHUNK, rows, half), f32),
            pltpu.VMEM((N_CHUNK, 2, 2, 2, rows, chunk), f32),
            pltpu.VMEM((N_CHUNK, rows, chunk), f32),
            pltpu.VMEM((rows, chunk), f32),
            pltpu.VMEM((rows, width), bf16),
            pltpu.VMEM((n_rows, ffn), f32),
            pltpu.VMEM((n_rows, ffn), f32),
            pltpu.VMEM((n_rows, ffn), bf16),
            pltpu.VMEM((N_SLOT, ffn, chunk), bf16),
            dma(()),
            dma((N_CHUNK,)),
            dma((N_SLOT,)),
            dma((5, N_CHUNK)),
            dma((5, N_CHUNK)),
            dma((5, N_CHUNK)),
            dma((5, N_CHUNK)),
        ],
        compiler_params=pltpu.CompilerParams(collective_id=0, has_side_effects=True,
                                             vmem_limit_bytes=67043328),
        name='layer_tail',
    )(attn_out, resid_in, gain_mlp.reshape(1, width), w_out, w_gate.T, w_up.T, w_down)


def solution(mesh):
    def layer_local(resid_in, positions, k_cache, v_cache, gain_attn, w_query, w_key, w_value,
                    w_out, gain_mlp, w_gate, w_up, w_down):
        attn_out, k_full, v_full = attention_block(resid_in, positions, k_cache, v_cache,
                                                   gain_attn, w_query, w_key, w_value)
        resid_out = layer_tail(attn_out, resid_in, gain_mlp, w_out, w_gate, w_up, w_down)
        return resid_out, k_full, v_full

    row_spec = P('dp', None)
    cache_spec = P('dp', None, 'tp', None)
    col_spec = P(None, 'tp')
    split_rows = P('tp', None)
    return jax.shard_map(layer_local, mesh=mesh,
                         in_specs=(row_spec, P('dp'), cache_spec, cache_spec, P(), col_spec, col_spec,
                                   col_spec, split_rows, P(), col_spec, col_spec, split_rows),
                         out_specs=(row_spec, cache_spec, cache_spec), check_vma=False)
```

```python
import math
import jax
import jax.numpy as jnp
from jax import lax
from jax.experimental import pallas as pl
from jax.experimental.pallas import tpu as pltpu
from jax.sharding import PartitionSpec as P

EPS = 1e-5
ROPE_THETA = 500000.0
ROPE_FACTOR = 8.0
LOW_FACTOR = 1.0
HIGH_FACTOR = 4.0
ORIG_CTX = 8192.0


def rope_freqs(head_dim):
    half_dim = head_dim // 2
    exponents = (jnp.arange(head_dim, dtype=jnp.int32) % half_dim).astype(jnp.float32) * (2.0 / head_dim)
    inv_freq = 1.0 / jnp.power(ROPE_THETA, exponents)
    wavelen = (2.0 * math.pi) / inv_freq
    smooth = (ORIG_CTX / wavelen - LOW_FACTOR) / (HIGH_FACTOR - LOW_FACTOR)
    blended = (1.0 - smooth) * inv_freq / ROPE_FACTOR + smooth * inv_freq
    inv_freq = jnp.where(wavelen < ORIG_CTX / HIGH_FACTOR, inv_freq,
                         jnp.where(wavelen > ORIG_CTX / LOW_FACTOR, inv_freq / ROPE_FACTOR, blended))
    return inv_freq[None, :]


def front_kernel(pos_ref, resid_ref, gain_ref, pos_row_ref, freq_ref, w_query_hbm, w_key_hbm, w_value_hbm,
                 k_in_hbm, v_in_hbm, attn_ref, k_out_hbm, v_out_hbm,
                 w_buf, acc, k_buf, v_buf, q_rows, o_rows, k_new, v_new, gain_f, cos_ref, sin_ref,
                 w_sem, cache_sem, out_sem):
    n_seqs, width = resid_ref.shape
    depth, q_width = w_buf.shape[1], w_query_hbm.shape[1]
    head_dim = k_new.shape[1]
    group_size = q_width // head_dim
    n_block = n_seqs // SEQ_BLOCK

    def w_copies(c):
        span = pl.ds(pl.multiple_of(c * depth, depth), depth)
        copies = []
        for i, (src, lo, size) in enumerate(((w_query_hbm, 0, q_width), (w_key_hbm, q_width, head_dim),
                                             (w_value_hbm, q_width + head_dim, head_dim))):
            copies.append(pltpu.make_async_copy(src.at[span], w_buf.at[c, :, pl.ds(lo, size)], w_sem.at[i, c]))
        return copies

    def block(b):
        return pl.ds(pl.multiple_of(b * SEQ_BLOCK, SEQ_BLOCK), SEQ_BLOCK)

    def in_copies(b):
        return (pltpu.make_async_copy(k_in_hbm.at[block(b)], k_buf.at[block(b)], cache_sem.at[0, b]),
                pltpu.make_async_copy(v_in_hbm.at[block(b)], v_buf.at[block(b)], cache_sem.at[1, b]))

    def out_copies(b):
        return (pltpu.make_async_copy(k_buf.at[block(b)], k_out_hbm.at[block(b)], out_sem.at[0, b]),
                pltpu.make_async_copy(v_buf.at[block(b)], v_out_hbm.at[block(b)], out_sem.at[1, b]))

    n_w = width // depth
    for c in range(n_w):
        for copy in w_copies(c):
            copy.start()
    gain_f[...] = gain_ref[...].astype(jnp.float32)

    def cols(c):
        return pl.ds(pl.multiple_of(c * depth, depth), depth)

    def add_squares(c, total):
        part = resid_ref[:, cols(c)].astype(jnp.float32)
        part = part * part
        for j in range(depth // 128):
            total = total + part[:, j * 128:(j + 1) * 128]
        return total

    squares = lax.fori_loop(0, n_w, add_squares, jnp.zeros((n_seqs, 128), jnp.float32))
    scale = lax.rsqrt(jnp.sum(squares, axis=-1, keepdims=True) * (1.0 / width) + EPS)
    acc[...] = jnp.zeros_like(acc)
    angles = (jnp.broadcast_to(pos_row_ref[...].astype(jnp.float32), (n_seqs, n_seqs)).T[:, :1]
              * freq_ref[...])
    cos_f = jnp.cos(angles)
    sin_f = jnp.sin(angles)
    sin_f = jnp.where(lax.broadcasted_iota(jnp.int32, sin_f.shape, 1) < head_dim // 2, -sin_f, sin_f)
    cos_ref[...] = cos_f
    sin_ref[...] = sin_f
    per_step = n_block // (n_w // 2)

    def project(c, carry):
        rows_f = resid_ref[:, cols(c)].astype(jnp.float32) * scale
        normed = jnp.concatenate(
            [rows_f[:, j * 128:(j + 1) * 128] * gain_f[pl.ds(c * (depth // 128) + j, 1), :]
             for j in range(depth // 128)], axis=-1).astype(jnp.bfloat16)
        for copy in w_copies(c):
            copy.wait()

        @pl.when(c >= n_w // 2)
        def _():
            for i in range(per_step):
                for copy in in_copies((c - n_w // 2) * per_step + i):
                    copy.start()

        acc[...] += jnp.dot(normed, w_buf[c], preferred_element_type=jnp.float32)
        return carry

    lax.fori_loop(0, n_w, project, 0)

    def rotate(cols_f):
        values = cols_f.astype(jnp.bfloat16).astype(jnp.float32)
        turned = values * cos_ref[...] + pltpu.roll(values, head_dim // 2, 1) * sin_ref[...]
        return turned.astype(jnp.bfloat16).astype(jnp.float32)

    for j in range(group_size):
        q_rows[pl.ds(j, n_seqs, stride=group_size), :] = rotate(acc[:, j * head_dim:(j + 1) * head_dim])
    k_new[...] = rotate(acc[:, q_width:q_width + head_dim])
    v_new[...] = acc[:, q_width + head_dim:].astype(jnp.bfloat16).astype(jnp.float32)
    inv_sqrt = 1.0 / math.sqrt(head_dim)

    def attend(b, carry):
        for copy in in_copies(b):
            copy.wait()
        for i in range(SEQ_BLOCK):
            seq = b * SEQ_BLOCK + i
            pos = pos_ref[seq]
            base = pl.multiple_of(pos // 16 * 16, 16)
            hit = lax.broadcasted_iota(jnp.int32, (16, head_dim), 0) == pos - base
            for buf, new in ((k_buf, k_new), (v_buf, v_new)):
                old = buf[seq, pl.ds(base, 16), :].astype(jnp.float32)
                buf[seq, pl.ds(base, 16), :] = jnp.where(hit, new[pl.ds(seq, 1), :], old).astype(jnp.bfloat16)
        for copy in out_copies(b):
            copy.start()
        rows, probs = [], []
        for i in range(SEQ_BLOCK):
            seq = b * SEQ_BLOCK + i
            rows.append(pl.ds(pl.multiple_of(seq * group_size, group_size), group_size))
            query = q_rows[rows[i], :].astype(jnp.bfloat16)
            scores = lax.dot_general(query, k_buf[seq], (((1,), (1,)), ((), ())),
                                     preferred_element_type=jnp.float32) * inv_sqrt
            valid = lax.broadcasted_iota(jnp.int32, scores.shape, 1) <= pos_ref[seq]
            scores = jnp.where(valid, scores, -jnp.inf)
            exps = jnp.exp(scores - jnp.max(scores, axis=-1, keepdims=True))
            probs.append((exps / jnp.sum(exps, axis=-1, keepdims=True)).astype(jnp.bfloat16))
        for i in range(SEQ_BLOCK):
            o_rows[rows[i], :] = jnp.dot(probs[i], v_buf[b * SEQ_BLOCK + i], preferred_element_type=jnp.float32)
        return carry

    lax.fori_loop(0, n_block, attend, 0)
    for j in range(group_size):
        attn_ref[:, j * head_dim:(j + 1) * head_dim] = (
            o_rows[pl.ds(j, n_seqs, stride=group_size), :].astype(jnp.bfloat16))
    for b in range(n_block):
        for copy in out_copies(b):
            copy.wait()


SEQ_BLOCK = 16
FRONT_DEPTH = 1024


def layer_front(resid_in, positions, k_cache, v_cache, gain_attn, w_query, w_key, w_value):
    n_seqs, width = resid_in.shape
    cache_len, head_dim = k_cache.shape[1], k_cache.shape[3]
    q_width = w_query.shape[1]
    f32, bf16 = jnp.float32, jnp.bfloat16
    vmem = pl.BlockSpec(memory_space=pltpu.VMEM)
    hbm = pl.BlockSpec(memory_space=pl.ANY)
    dma = pltpu.SemaphoreType.DMA
    n_w, n_block = width // FRONT_DEPTH, n_seqs // SEQ_BLOCK
    flat = (n_seqs, cache_len, head_dim)
    attn_out, k_out, v_out = pl.pallas_call(
        front_kernel,
        out_shape=(jax.ShapeDtypeStruct((n_seqs, q_width), bf16),
                   jax.ShapeDtypeStruct(flat, bf16), jax.ShapeDtypeStruct(flat, bf16)),
        in_specs=[pl.BlockSpec(memory_space=pltpu.SMEM), vmem, vmem, vmem, vmem, hbm, hbm, hbm, hbm, hbm],
        out_specs=(vmem, hbm, hbm),
        scratch_shapes=[
            pltpu.VMEM((n_w, FRONT_DEPTH, q_width + 2 * head_dim), bf16),
            pltpu.VMEM((n_seqs, q_width + 2 * head_dim), f32),
            pltpu.VMEM(flat, bf16),
            pltpu.VMEM(flat, bf16),
            pltpu.VMEM((n_seqs * q_width // head_dim, head_dim), f32),
            pltpu.VMEM((n_seqs * q_width // head_dim, head_dim), f32),
            pltpu.VMEM((n_seqs, head_dim), f32),
            pltpu.VMEM((n_seqs, head_dim), f32),
            pltpu.VMEM((width // 128, 128), f32),
            pltpu.VMEM((n_seqs, head_dim), f32),
            pltpu.VMEM((n_seqs, head_dim), f32),
            dma((3, n_w)),
            dma((2, n_block)),
            dma((2, n_block)),
        ],
        compiler_params=pltpu.CompilerParams(vmem_limit_bytes=67043328),
        name='layer_front',
    )(positions, resid_in, gain_attn.reshape(width // 128, 128), positions[None, :],
      rope_freqs(head_dim), w_query, w_key, w_value,
      k_cache.reshape(flat), v_cache.reshape(flat))
    return attn_out, k_out.reshape(k_cache.shape), v_out.reshape(v_cache.shape)


N_CHUNK = 16
N_SLOT = 15
MESH = pl.DeviceIdType.MESH


def tail_kernel(attn_ref, resid_hbm, gain_ref, w_out_hbm, gate_t_hbm, up_t_hbm, w_down_hbm, out_ref,
                part, from_core, from_x1, from_y1, from_x2, from_y2, gathered, mid, sq_sum, resid_own, gain_f,
                gate_acc, up_acc, hidden, ring,
                resid_sem, out_sem, ring_sem, rs_send, rs_recv, ag_send, ag_recv):
    n_chunk, chunk = N_CHUNK, part.shape[-1]
    half = chunk // 2
    rows = mid.shape[1]
    me = lax.axis_index('tp')
    k = me % 2
    x = (me // 2) % 2
    y = me // 4
    nk, nx, ny = 1 - k, 1 - x, 1 - y
    core_nbr = {'tp': me + 1 - 2 * k}
    x_nbr = {'tp': me + 2 - 4 * x}
    y_nbr = {'tp': me + 4 - 8 * y}

    def cols(c):
        return pl.ds(pl.multiple_of(c * chunk, chunk), chunk)

    depth_out = w_out_hbm.shape[0]
    first_mlp = n_chunk // 2
    first_down = first_mlp + 2 * n_chunk

    def out_slot(c):
        return c // 2, pl.ds(pl.multiple_of((c % 2) * depth_out, depth_out), depth_out)

    def out_copy(c):
        slot, span = out_slot(c)
        return pltpu.make_async_copy(w_out_hbm.at[:, cols(c)], ring.at[slot, span], out_sem.at[c])

    def ring_copy(src, c, j):
        slot = j % N_SLOT
        return pltpu.make_async_copy(src.at[:, cols(c)], ring.at[slot], ring_sem.at[slot])

    def gate_copy(c):
        return ring_copy(gate_t_hbm, c, first_mlp + 2 * c)

    def up_copy(c):
        return ring_copy(up_t_hbm, c, first_mlp + 2 * c + 1)

    def down_copy(c):
        return ring_copy(w_down_hbm, c, first_down + c)

    def start_load(j):
        m = j - first_mlp

        @pl.when(j < first_down)
        def _():
            @pl.when(m % 2 == 0)
            def _():
                gate_copy(m // 2).start()

            @pl.when(m % 2 == 1)
            def _():
                up_copy(m // 2).start()

        @pl.when(jnp.logical_and(j >= first_down, j < first_down + n_chunk))
        def _():
            down_copy(j - first_down).start()

    row0 = pl.multiple_of(64 * k + 32 * x + 16 * y, 16)
    resid_copy = pltpu.make_async_copy(resid_hbm.at[pl.ds(row0, rows)], resid_own, resid_sem)
    resid_copy.start()
    for c in range(OUT_AHEAD):
        out_copy(c).start()

    barrier = pltpu.get_barrier_semaphore()
    for nbr in (core_nbr, x_nbr, y_nbr):
        pl.semaphore_signal(barrier, inc=1, device_id=nbr, device_id_type=MESH)

    def remote(src, dst, sems, ch, c, nbr):
        return pltpu.make_async_remote_copy(src_ref=src, dst_ref=dst, send_sem=sems[0].at[ch, c],
                                            recv_sem=sems[1].at[ch, c], device_id=nbr, device_id_type=MESH)

    rs = (rs_send, rs_recv)
    ag = (ag_send, ag_recv)
    left, right = pl.ds(0, half), pl.ds(half, half)

    def rs_core(c):
        return remote(part.at[c, nk], from_core.at[c], rs, 0, c, core_nbr)

    def rs_x1(c):
        return remote(part.at[c, k, nx, :, :, left], from_x1.at[c], rs, 1, c, x_nbr)

    def rs_y1(c):
        return remote(part.at[c, k, :, ny, :, right], from_y1.at[c], rs, 2, c, y_nbr)

    def rs_y2(c):
        return remote(part.at[c, k, x, ny, :, left], from_y2.at[c], rs, 3, c, y_nbr)

    def rs_x2(c):
        return remote(part.at[c, k, nx, y, :, right], from_x2.at[c], rs, 4, c, x_nbr)

    def ag_x(c):
        blk = gathered.at[c, k, x, y]
        return remote(blk, blk, ag, 0, c, x_nbr)

    def ag_y(c):
        blk = gathered.at[c, k, x, y]
        return remote(blk, blk, ag, 1, c, y_nbr)

    def ag_fwd_y(c):
        blk = gathered.at[c, k, nx, y, :, right]
        return remote(blk, blk, ag, 2, c, y_nbr)

    def ag_fwd_x(c):
        blk = gathered.at[c, k, x, ny, :, left]
        return remote(blk, blk, ag, 3, c, x_nbr)

    def ag_core(c):
        blk = gathered.at[c, k]
        return remote(blk, blk, ag, 4, c, core_nbr)

    def stage(s, lag, fn):
        c = s - lag

        @pl.when(jnp.logical_and(c >= 0, c < n_chunk))
        def _():
            fn(c)

    def rs_stage1(c):
        rs_core(c).wait_recv()
        part[c, k] = part[c, k] + from_core[c]
        rs_x1(c).start()
        rs_y1(c).start()

    def rs_stage2(c):
        rs_x1(c).wait_recv()
        part[c, k, x, :, :, left] = part[c, k, x, :, :, left] + from_x1[c]
        rs_y2(c).start()
        rs_y1(c).wait_recv()
        part[c, k, :, y, :, right] = part[c, k, :, y, :, right] + from_y1[c]
        rs_x2(c).start()

    def rs_stage3(c):
        rs_y2(c).wait_recv()
        rs_x2(c).wait_recv()
        total = jnp.concatenate([part[c, k, x, y, :, left] + from_y2[c],
                                 part[c, k, x, y, :, right] + from_x2[c]], axis=-1)
        for copy in (rs_core, rs_x1, rs_y1, rs_y2, rs_x2):
            copy(c).wait_send()
        return total

    def ag_stage1(c):
        ag_x(c).wait_recv()
        ag_fwd_y(c).start()
        ag_y(c).wait_recv()
        ag_fwd_x(c).start()

    def ag_stage2(c):
        ag_fwd_x(c).wait_recv()
        ag_fwd_y(c).wait_recv()
        ag_core(c).start()

    def ag_stage3(c):
        ag_core(c).wait_recv()
        block = gathered[c].reshape(8 * rows, chunk)
        for copy in (ag_x, ag_y, ag_fwd_x, ag_fwd_y, ag_core):
            copy(c).wait_send()
        return block

    gain_f[...] = gain_ref[...].astype(jnp.float32)
    sq_sum[...] = jnp.zeros_like(sq_sum)
    gate_acc[...] = jnp.zeros_like(gate_acc)
    up_acc[...] = jnp.zeros_like(up_acc)
    resid_copy.wait()
    pl.semaphore_wait(barrier, 3)

    def proj(c):
        out_copy(c).wait()
        slot, span = out_slot(c)
        res = jnp.dot(attn_ref[...], ring[slot, span], preferred_element_type=jnp.float32)
        part[c] = res.reshape(part.shape[1:])
        rs_core(c).start()

        @pl.when(c + OUT_AHEAD < n_chunk)
        def _():
            out_copy(c + OUT_AHEAD).start()

        @pl.when(first_mlp + c < N_SLOT)
        def _():
            start_load(first_mlp + c)

        @pl.when(c % 2 == 1)
        def _():
            start_load(c // 2 + N_SLOT)

    def finish_mid(c):
        total = rs_stage3(c)
        x1 = (resid_own[:, cols(c)].astype(jnp.float32) + total).astype(jnp.bfloat16).astype(jnp.float32)
        mid[c] = x1
        sq_sum[...] += x1 * x1

    def rs_body(s, carry):
        stage(s, RS1_LAG[2], finish_mid)
        stage(s, RS1_LAG[1], rs_stage2)
        stage(s, RS1_LAG[0], rs_stage1)
        stage(s, 0, proj)
        return carry

    lax.fori_loop(0, n_chunk + RS1_LAG[2], rs_body, 0)

    mean_sq = jnp.sum(sq_sum[...], axis=-1, keepdims=True) * (1.0 / (n_chunk * chunk))
    scale = lax.rsqrt(mean_sq + EPS)

    def send_normed(c):
        gain = jnp.concatenate([gain_f[pl.ds(c * (chunk // 128) + j, 1), :] for j in range(chunk // 128)], axis=-1)
        normed = (mid[c] * scale * gain).astype(jnp.bfloat16)
        gathered[c, k, x, y] = normed.astype(jnp.float32)
        ag_x(c).start()
        ag_y(c).start()

    def gate_up(c):
        block = ag_stage3(c).astype(jnp.bfloat16)
        for copy, acc, j in ((gate_copy, gate_acc, first_mlp + 2 * c), (up_copy, up_acc, first_mlp + 2 * c + 1)):
            copy(c).wait()
            acc[...] += lax.dot_general(ring[j % N_SLOT], block, (((1,), (1,)), ((), ())),
                                        preferred_element_type=jnp.float32)
            start_load(j + N_SLOT)

    def ag_body(s, carry):
        stage(s, 0, send_normed)
        stage(s, AG1_LAG[0], ag_stage1)
        stage(s, AG1_LAG[1], ag_stage2)
        stage(s, AG1_LAG[2], gate_up)
        return carry

    lax.fori_loop(0, n_chunk + AG1_LAG[2], ag_body, 0)

    for lo in range(0, hidden.shape[1], 128):
        span = slice(lo, min(lo + 128, hidden.shape[1]))
        gate = gate_acc[span, :].astype(jnp.bfloat16).astype(jnp.float32)
        up = up_acc[span, :].astype(jnp.bfloat16).astype(jnp.float32)
        hidden[:, span] = (jax.nn.silu(gate) * up).T.astype(jnp.bfloat16)

    def down(c):
        down_copy(c).wait()
        j = first_down + c
        res = jnp.dot(hidden[...], ring[j % N_SLOT], preferred_element_type=jnp.float32)
        part[c] = res.reshape(part.shape[1:])
        rs_core(c).start()
        start_load(j + N_SLOT)

    def finish_out(c):
        total = rs_stage3(c)
        gathered[c, k, x, y] = (mid[c] + total).astype(jnp.bfloat16).astype(jnp.float32)
        ag_x(c).start()
        ag_y(c).start()

    def store_out(c):
        out_ref[:, cols(c)] = ag_stage3(c).astype(jnp.bfloat16)

    base = RS2_LAG[2]

    def down_body(s, carry):
        stage(s, base + AG2_LAG[1], ag_stage2)
        stage(s, base + AG2_LAG[0], ag_stage1)
        stage(s, base, finish_out)
        stage(s, RS2_LAG[1], rs_stage2)
        stage(s, RS2_LAG[0], rs_stage1)
        stage(s, 0, down)
        stage(s, base + AG2_LAG[2], store_out)
        return carry

    lax.fori_loop(0, n_chunk + base + AG2_LAG[2], down_body, 0)


RS1_LAG = (2, 5, 7)
AG1_LAG = (2, 4, 5)
RS2_LAG = (2, 4, 6)
AG2_LAG = (2, 4, 5)
OUT_AHEAD = 5


def layer_tail(attn_out, resid_in, gain_mlp, w_out, w_gate, w_up, w_down):
    n_rows, width = resid_in.shape
    ffn = w_gate.shape[1]
    chunk = width // N_CHUNK
    half = chunk // 2
    rows = n_rows // 8
    f32, bf16 = jnp.float32, jnp.bfloat16
    vmem = pl.BlockSpec(memory_space=pltpu.VMEM)
    hbm = pl.BlockSpec(memory_space=pl.ANY)
    dma = pltpu.SemaphoreType.DMA
    return pl.pallas_call(
        tail_kernel,
        out_shape=jax.ShapeDtypeStruct((n_rows, width), bf16),
        in_specs=[vmem, hbm, vmem, hbm, hbm, hbm, hbm],
        out_specs=vmem,
        scratch_shapes=[
            pltpu.VMEM((N_CHUNK, 2, 2, 2, rows, chunk), f32),
            pltpu.VMEM((N_CHUNK, 2, 2, rows, chunk), f32),
            pltpu.VMEM((N_CHUNK, 2, rows, half), f32),
            pltpu.VMEM((N_CHUNK, 2, rows, half), f32),
            pltpu.VMEM((N_CHUNK, rows, half), f32),
            pltpu.VMEM((N_CHUNK, rows, half), f32),
            pltpu.VMEM((N_CHUNK, 2, 2, 2, rows, chunk), f32),
            pltpu.VMEM((N_CHUNK, rows, chunk), f32),
            pltpu.VMEM((rows, chunk), f32),
            pltpu.VMEM((rows, width), bf16),
            pltpu.VMEM((width // 128, 128), f32),
            pltpu.VMEM((ffn, n_rows), f32),
            pltpu.VMEM((ffn, n_rows), f32),
            pltpu.VMEM((n_rows, ffn), bf16),
            pltpu.VMEM((N_SLOT, ffn, chunk), bf16),
            dma(()),
            dma((N_CHUNK,)),
            dma((N_SLOT,)),
            dma((5, N_CHUNK)),
            dma((5, N_CHUNK)),
            dma((5, N_CHUNK)),
            dma((5, N_CHUNK)),
        ],
        compiler_params=pltpu.CompilerParams(collective_id=0, has_side_effects=True,
                                             vmem_limit_bytes=67043328),
        name='layer_tail',
    )(attn_out, resid_in, gain_mlp.reshape(width // 128, 128), w_out, w_gate.T, w_up.T, w_down)


def solution(mesh):
    def layer_local(resid_in, positions, k_cache, v_cache, gain_attn, w_query, w_key, w_value,
                    w_out, gain_mlp, w_gate, w_up, w_down):
        attn_out, k_full, v_full = layer_front(resid_in, positions, k_cache, v_cache,
                                               gain_attn, w_query, w_key, w_value)
        resid_out = layer_tail(attn_out, resid_in, gain_mlp, w_out, w_gate, w_up, w_down)
        return resid_out, k_full, v_full

    row_spec = P('dp', None)
    cache_spec = P('dp', None, 'tp', None)
    col_spec = P(None, 'tp')
    split_rows = P('tp', None)
    return jax.shard_map(layer_local, mesh=mesh,
                         in_specs=(row_spec, P('dp'), cache_spec, cache_spec, P(), col_spec, col_spec,
                                   col_spec, split_rows, P(), col_spec, col_spec, split_rows),
                         out_specs=(row_spec, cache_spec, cache_spec), check_vma=False)
```

```python
import math
import jax
import jax.numpy as jnp
from jax import lax
from jax.experimental import pallas as pl
from jax.experimental.pallas import tpu as pltpu
from jax.sharding import PartitionSpec as P

EPS = 1e-5
ROPE_THETA = 500000.0
ROPE_FACTOR = 8.0
LOW_FACTOR = 1.0
HIGH_FACTOR = 4.0
ORIG_CTX = 8192.0


def rope_freqs(head_dim):
    half_dim = head_dim // 2
    exponents = (jnp.arange(head_dim, dtype=jnp.int32) % half_dim).astype(jnp.float32) * (2.0 / head_dim)
    inv_freq = 1.0 / jnp.power(ROPE_THETA, exponents)
    wavelen = (2.0 * math.pi) / inv_freq
    smooth = (ORIG_CTX / wavelen - LOW_FACTOR) / (HIGH_FACTOR - LOW_FACTOR)
    blended = (1.0 - smooth) * inv_freq / ROPE_FACTOR + smooth * inv_freq
    inv_freq = jnp.where(wavelen < ORIG_CTX / HIGH_FACTOR, inv_freq,
                         jnp.where(wavelen > ORIG_CTX / LOW_FACTOR, inv_freq / ROPE_FACTOR, blended))
    return inv_freq[None, :]


def front_kernel(pos_ref, resid_hbm, gain_ref, pos_row_ref, freq_ref, w_query_hbm, w_key_hbm, w_value_hbm,
                 k_in_hbm, v_in_hbm, attn_ref, k_out_hbm, v_out_hbm,
                 w_buf, acc, k_buf, v_buf, q_rows, o_rows, k_new, v_new, gain_f, cos_ref, sin_ref, resid_ref,
                 resid_sem, w_sem, cache_sem, out_sem):
    n_seqs, width = resid_ref.shape
    depth, q_width = w_buf.shape[1], w_query_hbm.shape[1]
    head_dim = k_new.shape[1]
    group_size = q_width // head_dim
    n_block = n_seqs // SEQ_BLOCK

    def w_copies(c):
        span = pl.ds(pl.multiple_of(c * depth, depth), depth)
        copies = []
        for i, (src, lo, size) in enumerate(((w_query_hbm, 0, q_width), (w_key_hbm, q_width, head_dim),
                                             (w_value_hbm, q_width + head_dim, head_dim))):
            copies.append(pltpu.make_async_copy(src.at[span], w_buf.at[c, :, pl.ds(lo, size)], w_sem.at[i, c]))
        return copies

    def block(b):
        return pl.ds(pl.multiple_of(b * SEQ_BLOCK, SEQ_BLOCK), SEQ_BLOCK)

    def in_copies(b):
        return (pltpu.make_async_copy(k_in_hbm.at[block(b)], k_buf.at[block(b)], cache_sem.at[0, b]),
                pltpu.make_async_copy(v_in_hbm.at[block(b)], v_buf.at[block(b)], cache_sem.at[1, b]))

    def out_copies(b):
        return (pltpu.make_async_copy(k_buf.at[block(b)], k_out_hbm.at[block(b)], out_sem.at[0, b]),
                pltpu.make_async_copy(v_buf.at[block(b)], v_out_hbm.at[block(b)], out_sem.at[1, b]))

    n_w = width // depth
    resid_copy = pltpu.make_async_copy(resid_hbm, resid_ref, resid_sem)
    resid_copy.start()
    for c in range(n_w):
        for copy in w_copies(c):
            copy.start()
    gain_f[...] = gain_ref[...].astype(jnp.float32)

    def cols(c):
        return pl.ds(pl.multiple_of(c * depth, depth), depth)

    def add_squares(c, total):
        part = resid_ref[:, cols(c)].astype(jnp.float32)
        part = part * part
        for j in range(depth // 128):
            total = total + part[:, j * 128:(j + 1) * 128]
        return total

    acc[...] = jnp.zeros_like(acc)
    angles = (jnp.broadcast_to(pos_row_ref[...].astype(jnp.float32), (n_seqs, n_seqs)).T[:, :1]
              * freq_ref[...])
    cos_f = jnp.cos(angles)
    sin_f = jnp.sin(angles)
    sin_f = jnp.where(lax.broadcasted_iota(jnp.int32, sin_f.shape, 1) < head_dim // 2, -sin_f, sin_f)
    cos_ref[...] = cos_f
    sin_ref[...] = sin_f
    with jax.named_scope('wait_resid'):
        resid_copy.wait()
    squares = lax.fori_loop(0, n_w, add_squares, jnp.zeros((n_seqs, 128), jnp.float32))
    scale = lax.rsqrt(jnp.sum(squares, axis=-1, keepdims=True) * (1.0 / width) + EPS)
    per_step = n_block // (n_w // 2)

    def project(c, carry):
        rows_f = resid_ref[:, cols(c)].astype(jnp.float32) * scale
        normed = jnp.concatenate(
            [rows_f[:, j * 128:(j + 1) * 128] * gain_f[pl.ds(c * (depth // 128) + j, 1), :]
             for j in range(depth // 128)], axis=-1).astype(jnp.bfloat16)
        for copy in w_copies(c):
            copy.wait()

        @pl.when(c >= n_w // 2)
        def _():
            for i in range(per_step):
                for copy in in_copies((c - n_w // 2) * per_step + i):
                    copy.start()

        acc[...] += jnp.dot(normed, w_buf[c], preferred_element_type=jnp.float32)
        return carry

    with jax.named_scope('project'):
        lax.fori_loop(0, n_w, project, 0)

    def rotate(cols_f):
        values = cols_f.astype(jnp.bfloat16).astype(jnp.float32)
        turned = values * cos_ref[...] + pltpu.roll(values, head_dim // 2, 1) * sin_ref[...]
        return turned.astype(jnp.bfloat16).astype(jnp.float32)

    for j in range(group_size):
        q_rows[pl.ds(j, n_seqs, stride=group_size), :] = rotate(acc[:, j * head_dim:(j + 1) * head_dim])
    k_new[...] = rotate(acc[:, q_width:q_width + head_dim])
    v_new[...] = acc[:, q_width + head_dim:].astype(jnp.bfloat16).astype(jnp.float32)
    inv_sqrt = 1.0 / math.sqrt(head_dim)

    def attend(b, carry):
        for copy in in_copies(b):
            copy.wait()
        for i in range(SEQ_BLOCK):
            seq = b * SEQ_BLOCK + i
            pos = pos_ref[seq]
            base = pl.multiple_of(pos // 16 * 16, 16)
            hit = lax.broadcasted_iota(jnp.int32, (16, head_dim), 0) == pos - base
            for buf, new in ((k_buf, k_new), (v_buf, v_new)):
                old = buf[seq, pl.ds(base, 16), :].astype(jnp.float32)
                buf[seq, pl.ds(base, 16), :] = jnp.where(hit, new[pl.ds(seq, 1), :], old).astype(jnp.bfloat16)
        for copy in out_copies(b):
            copy.start()
        rows, probs = [], []
        for i in range(SEQ_BLOCK):
            seq = b * SEQ_BLOCK + i
            rows.append(pl.ds(pl.multiple_of(seq * group_size, group_size), group_size))
            query = q_rows[rows[i], :].astype(jnp.bfloat16)
            scores = lax.dot_general(query, k_buf[seq], (((1,), (1,)), ((), ())),
                                     preferred_element_type=jnp.float32) * inv_sqrt
            valid = lax.broadcasted_iota(jnp.int32, scores.shape, 1) <= pos_ref[seq]
            scores = jnp.where(valid, scores, -jnp.inf)
            exps = jnp.exp(scores - jnp.max(scores, axis=-1, keepdims=True))
            probs.append((exps / jnp.sum(exps, axis=-1, keepdims=True)).astype(jnp.bfloat16))
        for i in range(SEQ_BLOCK):
            o_rows[rows[i], :] = jnp.dot(probs[i], v_buf[b * SEQ_BLOCK + i], preferred_element_type=jnp.float32)
        return carry

    with jax.named_scope('attend'):
        lax.fori_loop(0, n_block, attend, 0)
    for j in range(group_size):
        attn_ref[:, j * head_dim:(j + 1) * head_dim] = (
            o_rows[pl.ds(j, n_seqs, stride=group_size), :].astype(jnp.bfloat16))
    for b in range(n_block):
        for copy in out_copies(b):
            copy.wait()


SEQ_BLOCK = 32
FRONT_DEPTH = 1024


def layer_front(resid_in, positions, k_cache, v_cache, gain_attn, w_query, w_key, w_value):
    n_seqs, width = resid_in.shape
    cache_len, head_dim = k_cache.shape[1], k_cache.shape[3]
    q_width = w_query.shape[1]
    f32, bf16 = jnp.float32, jnp.bfloat16
    vmem = pl.BlockSpec(memory_space=pltpu.VMEM)
    hbm = pl.BlockSpec(memory_space=pl.ANY)
    dma = pltpu.SemaphoreType.DMA
    n_w, n_block = width // FRONT_DEPTH, n_seqs // SEQ_BLOCK
    flat = (n_seqs, cache_len, head_dim)
    attn_out, k_out, v_out = pl.pallas_call(
        front_kernel,
        out_shape=(jax.ShapeDtypeStruct((n_seqs, q_width), bf16),
                   jax.ShapeDtypeStruct(flat, bf16), jax.ShapeDtypeStruct(flat, bf16)),
        in_specs=[pl.BlockSpec(memory_space=pltpu.SMEM), hbm, vmem, vmem, vmem, hbm, hbm, hbm, hbm, hbm],
        out_specs=(vmem, hbm, hbm),
        scratch_shapes=[
            pltpu.VMEM((n_w, FRONT_DEPTH, q_width + 2 * head_dim), bf16),
            pltpu.VMEM((n_seqs, q_width + 2 * head_dim), f32),
            pltpu.VMEM(flat, bf16),
            pltpu.VMEM(flat, bf16),
            pltpu.VMEM((n_seqs * q_width // head_dim, head_dim), f32),
            pltpu.VMEM((n_seqs * q_width // head_dim, head_dim), f32),
            pltpu.VMEM((n_seqs, head_dim), f32),
            pltpu.VMEM((n_seqs, head_dim), f32),
            pltpu.VMEM((width // 128, 128), f32),
            pltpu.VMEM((n_seqs, head_dim), f32),
            pltpu.VMEM((n_seqs, head_dim), f32),
            pltpu.VMEM((n_seqs, width), bf16),
            dma(()),
            dma((3, n_w)),
            dma((2, n_block)),
            dma((2, n_block)),
        ],
        compiler_params=pltpu.CompilerParams(vmem_limit_bytes=67043328),
        name='layer_front',
    )(positions, resid_in, gain_attn.reshape(width // 128, 128), positions[None, :],
      rope_freqs(head_dim), w_query, w_key, w_value,
      k_cache.reshape(flat), v_cache.reshape(flat))
    return attn_out, k_out.reshape(k_cache.shape), v_out.reshape(v_cache.shape)


N_CHUNK = 16
SEND_SLOT = 8
N_SLOT = 11
T_ROWS = 1280
MESH = pl.DeviceIdType.MESH


def tail_kernel(attn_ref, resid_hbm, gain_ref, w_out_hbm, gate_t_hbm, up_t_hbm, w_down_hbm, out_ref,
                part, from_core, from_x1, from_y1, from_x2, from_y2, gathered, mid, sq_sum, resid_own, gain_f,
                gate_acc, up_acc, gate_acc_t, up_acc_t, turned, hidden, ring,
                resid_sem, out_sem, ring_sem, rs_send, rs_recv, ag_send, ag_recv):
    n_chunk, chunk = N_CHUNK, part.shape[-1]
    half = chunk // 2
    rows = mid.shape[1]
    me = lax.axis_index('tp')
    k = me % 2
    x = (me // 2) % 2
    y = me // 4
    nk, nx, ny = 1 - k, 1 - x, 1 - y
    core_nbr = {'tp': me + 1 - 2 * k}
    x_nbr = {'tp': me + 2 - 4 * x}
    y_nbr = {'tp': me + 4 - 8 * y}

    def cols(c):
        return pl.ds(pl.multiple_of(c * chunk, chunk), chunk)

    depth_out = w_out_hbm.shape[0]
    first_mlp = n_chunk // 2
    first_down = first_mlp + 2 * n_chunk

    def out_slot(c):
        return c // 2, pl.ds(pl.multiple_of((c % 2) * depth_out, depth_out), depth_out)

    def out_copy(c):
        slot, span = out_slot(c)
        return pltpu.make_async_copy(w_out_hbm.at[:, cols(c)], ring.at[slot, span], out_sem.at[c])

    def ring_copy(src, c, j):
        slot = j % N_SLOT
        return pltpu.make_async_copy(src.at[:, cols(c)], ring.at[slot], ring_sem.at[slot])

    def gate_copy(c):
        return ring_copy(gate_t_hbm, c, first_mlp + 2 * c)

    def up_copy(c):
        return ring_copy(up_t_hbm, c, first_mlp + 2 * c + 1)

    def down_copy(c):
        return ring_copy(w_down_hbm, c, first_down + c)

    def start_load(j):
        m = j - first_mlp

        @pl.when(j < first_down)
        def _():
            @pl.when(m % 2 == 0)
            def _():
                gate_copy(m // 2).start()

            @pl.when(m % 2 == 1)
            def _():
                up_copy(m // 2).start()

        @pl.when(jnp.logical_and(j >= first_down, j < first_down + n_chunk))
        def _():
            down_copy(j - first_down).start()

    row0 = pl.multiple_of(64 * k + 32 * x + 16 * y, 16)
    resid_copy = pltpu.make_async_copy(resid_hbm.at[pl.ds(row0, rows)], resid_own, resid_sem)
    resid_copy.start()
    for c in range(OUT_AHEAD):
        out_copy(c).start()

    barrier = pltpu.get_barrier_semaphore()
    for nbr in (core_nbr, x_nbr, y_nbr):
        pl.semaphore_signal(barrier, inc=1, device_id=nbr, device_id_type=MESH)

    def remote(src, dst, sems, ch, c, nbr):
        return pltpu.make_async_remote_copy(src_ref=src, dst_ref=dst, send_sem=sems[0].at[ch, c % SEND_SLOT],
                                            recv_sem=sems[1].at[ch, c], device_id=nbr, device_id_type=MESH)

    rs = (rs_send, rs_recv)
    ag = (ag_send, ag_recv)
    left, right = pl.ds(0, half), pl.ds(half, half)

    def rs_core(c):
        return remote(part.at[c, nk], from_core.at[c], rs, 0, c, core_nbr)

    def rs_x1(c):
        return remote(part.at[c, k, nx, :, :, left], from_x1.at[c], rs, 1, c, x_nbr)

    def rs_y1(c):
        return remote(part.at[c, k, :, ny, :, right], from_y1.at[c], rs, 2, c, y_nbr)

    def rs_y2(c):
        return remote(part.at[c, k, x, ny, :, left], from_y2.at[c], rs, 3, c, y_nbr)

    def rs_x2(c):
        return remote(part.at[c, k, nx, y, :, right], from_x2.at[c], rs, 4, c, x_nbr)

    def ag_x(c):
        blk = gathered.at[c, k, x, y]
        return remote(blk, blk, ag, 0, c, x_nbr)

    def ag_y(c):
        blk = gathered.at[c, k, x, y]
        return remote(blk, blk, ag, 1, c, y_nbr)

    def ag_fwd_y(c):
        blk = gathered.at[c, k, nx, y, :, right]
        return remote(blk, blk, ag, 2, c, y_nbr)

    def ag_fwd_x(c):
        blk = gathered.at[c, k, x, ny, :, left]
        return remote(blk, blk, ag, 3, c, x_nbr)

    def ag_core(c):
        blk = gathered.at[c, k]
        return remote(blk, blk, ag, 4, c, core_nbr)

    def stage(s, lag, fn):
        c = s - lag

        @pl.when(jnp.logical_and(c >= 0, c < n_chunk))
        def _():
            with jax.named_scope(fn.__name__):
                fn(c)

    def rs_stage1(c):
        rs_core(c).wait_recv()
        part[c, k] = part[c, k] + from_core[c]
        rs_x1(c).start()
        rs_y1(c).start()

    def rs_stage2(c):
        rs_x1(c).wait_recv()
        part[c, k, x, :, :, left] = part[c, k, x, :, :, left] + from_x1[c]
        rs_y2(c).start()
        rs_y1(c).wait_recv()
        part[c, k, :, y, :, right] = part[c, k, :, y, :, right] + from_y1[c]
        rs_x2(c).start()

    def rs_stage3(c):
        rs_y2(c).wait_recv()
        rs_x2(c).wait_recv()
        total = jnp.concatenate([part[c, k, x, y, :, left] + from_y2[c],
                                 part[c, k, x, y, :, right] + from_x2[c]], axis=-1)
        for copy in (rs_core, rs_x1, rs_y1, rs_y2, rs_x2):
            copy(c).wait_send()
        return total

    def ag_stage1(c):
        ag_x(c).wait_recv()
        ag_fwd_y(c).start()
        ag_y(c).wait_recv()
        ag_fwd_x(c).start()

    def ag_stage2(c):
        ag_fwd_x(c).wait_recv()
        ag_fwd_y(c).wait_recv()
        ag_core(c).start()

    def ag_stage3(c):
        ag_core(c).wait_recv()
        block = gathered[c].reshape(8 * rows, chunk)
        for copy in (ag_x, ag_y, ag_fwd_x, ag_fwd_y, ag_core):
            copy(c).wait_send()
        return block

    gain_f[...] = gain_ref[...].astype(jnp.float32)
    sq_sum[...] = jnp.zeros_like(sq_sum)
    gate_acc[...] = jnp.zeros_like(gate_acc)
    up_acc[...] = jnp.zeros_like(up_acc)
    gate_acc_t[...] = jnp.zeros_like(gate_acc_t)
    up_acc_t[...] = jnp.zeros_like(up_acc_t)
    resid_copy.wait()
    with jax.named_scope('entry_barrier'):
        pl.semaphore_wait(barrier, 3)

    def proj(c):
        out_copy(c).wait()
        slot, span = out_slot(c)
        res = jnp.dot(attn_ref[...], ring[slot, span], preferred_element_type=jnp.float32)
        part[c] = res.reshape(part.shape[1:])
        rs_core(c).start()

        @pl.when(c + OUT_AHEAD < n_chunk)
        def _():
            out_copy(c + OUT_AHEAD).start()

        @pl.when(first_mlp + c < N_SLOT)
        def _():
            start_load(first_mlp + c)

        @pl.when(c % 2 == 1)
        def _():
            start_load(c // 2 + N_SLOT)

    def finish_mid(c):
        total = rs_stage3(c)
        x1 = (resid_own[:, cols(c)].astype(jnp.float32) + total).astype(jnp.bfloat16).astype(jnp.float32)
        mid[c] = x1
        sq_sum[...] += x1 * x1

    def rs_body(s, carry):
        stage(s, RS1_LAG[2], finish_mid)
        stage(s, RS1_LAG[1], rs_stage2)
        stage(s, RS1_LAG[0], rs_stage1)
        stage(s, 0, proj)
        return carry

    with jax.named_scope('phase_rs1'):
        lax.fori_loop(0, n_chunk + RS1_LAG[2], rs_body, 0)

    mean_sq = jnp.sum(sq_sum[...], axis=-1, keepdims=True) * (1.0 / (n_chunk * chunk))
    scale = lax.rsqrt(mean_sq + EPS)

    def send_normed(c):
        gain = jnp.concatenate([gain_f[pl.ds(c * (chunk // 128) + j, 1), :] for j in range(chunk // 128)], axis=-1)
        normed = (mid[c] * scale * gain).astype(jnp.bfloat16)
        gathered[c, k, x, y] = normed.astype(jnp.float32)
        ag_x(c).start()
        ag_y(c).start()

    def gate_up(c):
        block = ag_stage3(c).astype(jnp.bfloat16)
        gate_copy(c).wait()
        up_copy(c).wait()
        first = first_mlp + 2 * c
        accs = ((gate_acc, gate_acc_t), (up_acc, up_acc_t))
        for i, (acc, acc_t) in enumerate(accs):
            slot = (first + i) % N_SLOT
            turned[i] = ring[slot, pl.ds(T_ROWS, acc_t.shape[1])].T
            acc[...] += lax.dot_general(ring[slot, pl.ds(0, T_ROWS)], block, (((1,), (1,)), ((), ())),
                                        preferred_element_type=jnp.float32)
        for i, (acc, acc_t) in enumerate(accs):
            acc_t[...] += jnp.dot(block, turned[i], preferred_element_type=jnp.float32)
        for i in range(2):
            start_load(first + i + N_SLOT)

    def ag_body(s, carry):
        stage(s, 0, send_normed)
        stage(s, AG1_LAG[0], ag_stage1)
        stage(s, AG1_LAG[1], ag_stage2)
        stage(s, AG1_LAG[2], gate_up)
        return carry

    with jax.named_scope('phase_ag1'):
        lax.fori_loop(0, n_chunk + AG1_LAG[2], ag_body, 0)

    def act(gate, up):
        gate = gate.astype(jnp.bfloat16).astype(jnp.float32)
        up = up.astype(jnp.bfloat16).astype(jnp.float32)
        return jax.nn.silu(gate) * up

    for lo in range(0, T_ROWS, 128):
        span = slice(lo, lo + 128)
        hidden[:, span] = act(gate_acc[span, :], up_acc[span, :]).T.astype(jnp.bfloat16)
    hidden[:, T_ROWS:] = act(gate_acc_t[...], up_acc_t[...]).astype(jnp.bfloat16)

    def down(c):
        down_copy(c).wait()
        j = first_down + c
        res = jnp.dot(hidden[...], ring[j % N_SLOT], preferred_element_type=jnp.float32)
        part[c] = res.reshape(part.shape[1:])
        rs_core(c).start()
        start_load(j + N_SLOT)

    def finish_out(c):
        total = rs_stage3(c)
        gathered[c, k, x, y] = (mid[c] + total).astype(jnp.bfloat16).astype(jnp.float32)
        ag_x(c).start()
        ag_y(c).start()

    def store_out(c):
        out_ref[:, cols(c)] = ag_stage3(c).astype(jnp.bfloat16)

    base = RS2_LAG[2]

    def down_body(s, carry):
        stage(s, base + AG2_LAG[1], ag_stage2)
        stage(s, base + AG2_LAG[0], ag_stage1)
        stage(s, base, finish_out)
        stage(s, RS2_LAG[1], rs_stage2)
        stage(s, RS2_LAG[0], rs_stage1)
        stage(s, 0, down)
        stage(s, base + AG2_LAG[2], store_out)
        return carry

    with jax.named_scope('phase_ar2'):
        lax.fori_loop(0, n_chunk + base + AG2_LAG[2], down_body, 0)


RS1_LAG = (2, 5, 7)
AG1_LAG = (2, 4, 5)
RS2_LAG = (2, 4, 6)
AG2_LAG = (2, 4, 5)
OUT_AHEAD = 5


def layer_tail(attn_out, resid_in, gain_mlp, w_out, w_gate, w_up, w_down):
    n_rows, width = resid_in.shape
    ffn = w_gate.shape[1]
    chunk = width // N_CHUNK
    half = chunk // 2
    rows = n_rows // 8
    f32, bf16 = jnp.float32, jnp.bfloat16
    vmem = pl.BlockSpec(memory_space=pltpu.VMEM)
    hbm = pl.BlockSpec(memory_space=pl.ANY)
    dma = pltpu.SemaphoreType.DMA
    return pl.pallas_call(
        tail_kernel,
        out_shape=jax.ShapeDtypeStruct((n_rows, width), bf16),
        in_specs=[vmem, hbm, vmem, hbm, hbm, hbm, hbm],
        out_specs=vmem,
        scratch_shapes=[
            pltpu.VMEM((N_CHUNK, 2, 2, 2, rows, chunk), f32),
            pltpu.VMEM((N_CHUNK, 2, 2, rows, chunk), f32),
            pltpu.VMEM((N_CHUNK, 2, rows, half), f32),
            pltpu.VMEM((N_CHUNK, 2, rows, half), f32),
            pltpu.VMEM((N_CHUNK, rows, half), f32),
            pltpu.VMEM((N_CHUNK, rows, half), f32),
            pltpu.VMEM((N_CHUNK, 2, 2, 2, rows, chunk), f32),
            pltpu.VMEM((N_CHUNK, rows, chunk), f32),
            pltpu.VMEM((rows, chunk), f32),
            pltpu.VMEM((rows, width), bf16),
            pltpu.VMEM((width // 128, 128), f32),
            pltpu.VMEM((T_ROWS, n_rows), f32),
            pltpu.VMEM((T_ROWS, n_rows), f32),
            pltpu.VMEM((n_rows, ffn - T_ROWS), f32),
            pltpu.VMEM((n_rows, ffn - T_ROWS), f32),
            pltpu.VMEM((2, chunk, ffn - T_ROWS), bf16),
            pltpu.VMEM((n_rows, ffn), bf16),
            pltpu.VMEM((N_SLOT, ffn, chunk), bf16),
            dma(()),
            dma((N_CHUNK,)),
            dma((N_SLOT,)),
            dma((5, SEND_SLOT)),
            dma((5, N_CHUNK)),
            dma((5, SEND_SLOT)),
            dma((5, N_CHUNK)),
        ],
        compiler_params=pltpu.CompilerParams(collective_id=0, has_side_effects=True,
                                             vmem_limit_bytes=53477376),
        name='layer_tail',
    )(attn_out, resid_in, gain_mlp.reshape(width // 128, 128), w_out, w_gate.T, w_up.T, w_down)


def solution(mesh):
    def layer_local(resid_in, positions, k_cache, v_cache, gain_attn, w_query, w_key, w_value,
                    w_out, gain_mlp, w_gate, w_up, w_down):
        attn_out, k_full, v_full = layer_front(resid_in, positions, k_cache, v_cache,
                                               gain_attn, w_query, w_key, w_value)
        resid_out = layer_tail(attn_out, resid_in, gain_mlp, w_out, w_gate, w_up, w_down)
        return resid_out, k_full, v_full

    row_spec = P('dp', None)
    cache_spec = P('dp', None, 'tp', None)
    col_spec = P(None, 'tp')
    split_rows = P('tp', None)
    return jax.shard_map(layer_local, mesh=mesh,
                         in_specs=(row_spec, P('dp'), cache_spec, cache_spec, P(), col_spec, col_spec,
                                   col_spec, split_rows, P(), col_spec, col_spec, split_rows),
                         out_specs=(row_spec, cache_spec, cache_spec), check_vma=False)
```

```python
import math
import jax
import jax.numpy as jnp
from jax import lax
from jax.experimental import pallas as pl
from jax.experimental.pallas import tpu as pltpu
from jax.sharding import PartitionSpec as P

EPS = 1e-5
ROPE_THETA = 500000.0
ROPE_FACTOR = 8.0
LOW_FACTOR = 1.0
HIGH_FACTOR = 4.0
ORIG_CTX = 8192.0


def rope_freqs(head_dim):
    half_dim = head_dim // 2
    exponents = (jnp.arange(head_dim, dtype=jnp.int32) % half_dim).astype(jnp.float32) * (2.0 / head_dim)
    inv_freq = 1.0 / jnp.power(ROPE_THETA, exponents)
    wavelen = (2.0 * math.pi) / inv_freq
    smooth = (ORIG_CTX / wavelen - LOW_FACTOR) / (HIGH_FACTOR - LOW_FACTOR)
    blended = (1.0 - smooth) * inv_freq / ROPE_FACTOR + smooth * inv_freq
    inv_freq = jnp.where(wavelen < ORIG_CTX / HIGH_FACTOR, inv_freq,
                         jnp.where(wavelen > ORIG_CTX / LOW_FACTOR, inv_freq / ROPE_FACTOR, blended))
    return inv_freq[None, :]


def front_kernel(pos_ref, resid_hbm, gain_ref, pos_row_ref, freq_ref, w_query_hbm, w_key_hbm, w_value_hbm,
                 k_in_hbm, v_in_hbm, attn_ref, k_out_hbm, v_out_hbm,
                 w_buf, acc, k_buf, v_buf, q_rows, o_rows, k_new, v_new, gain_f, cos_ref, sin_ref, resid_ref,
                 resid_sem, w_sem, cache_sem, out_sem):
    n_seqs, width = resid_ref.shape
    depth, q_width = w_buf.shape[1], w_query_hbm.shape[1]
    head_dim = k_new.shape[1]
    group_size = q_width // head_dim
    n_block = n_seqs // SEQ_BLOCK

    def w_copies(c):
        span = pl.ds(pl.multiple_of(c * depth, depth), depth)
        copies = []
        for i, (src, lo, size) in enumerate(((w_query_hbm, 0, q_width), (w_key_hbm, q_width, head_dim),
                                             (w_value_hbm, q_width + head_dim, head_dim))):
            copies.append(pltpu.make_async_copy(src.at[span], w_buf.at[c, :, pl.ds(lo, size)], w_sem.at[i, c]))
        return copies

    def block(b):
        return pl.ds(pl.multiple_of(b * SEQ_BLOCK, SEQ_BLOCK), SEQ_BLOCK)

    def in_copies(b):
        return (pltpu.make_async_copy(k_in_hbm.at[block(b)], k_buf.at[block(b)], cache_sem.at[0, b]),
                pltpu.make_async_copy(v_in_hbm.at[block(b)], v_buf.at[block(b)], cache_sem.at[1, b]))

    def out_copies(b):
        return (pltpu.make_async_copy(k_buf.at[block(b)], k_out_hbm.at[block(b)], out_sem.at[0, b]),
                pltpu.make_async_copy(v_buf.at[block(b)], v_out_hbm.at[block(b)], out_sem.at[1, b]))

    n_w = width // depth
    resid_copy = pltpu.make_async_copy(resid_hbm, resid_ref, resid_sem)
    resid_copy.start()
    for c in range(2):
        for copy in w_copies(c):
            copy.start()
    gain_f[...] = gain_ref[...].astype(jnp.float32)

    def cols(c):
        return pl.ds(pl.multiple_of(c * depth, depth), depth)

    def add_squares(c, total):
        part = resid_ref[:, cols(c)].astype(jnp.float32)
        part = part * part
        for j in range(depth // 128):
            total = total + part[:, j * 128:(j + 1) * 128]
        return total

    acc[...] = jnp.zeros_like(acc)
    angles = (jnp.broadcast_to(pos_row_ref[...].astype(jnp.float32), (n_seqs, n_seqs)).T[:, :1]
              * freq_ref[...])
    cos_f = jnp.cos(angles)
    sin_f = jnp.sin(angles)
    sin_f = jnp.where(lax.broadcasted_iota(jnp.int32, sin_f.shape, 1) < head_dim // 2, -sin_f, sin_f)
    cos_ref[...] = cos_f
    sin_ref[...] = sin_f
    with jax.named_scope('wait_resid'):
        resid_copy.wait()
    for c in range(2, W_AHEAD):
        for copy in w_copies(c):
            copy.start()
    squares = lax.fori_loop(0, n_w, add_squares, jnp.zeros((n_seqs, 128), jnp.float32))
    scale = lax.rsqrt(jnp.sum(squares, axis=-1, keepdims=True) * (1.0 / width) + EPS)
    per_step = n_block // (n_w // 2)

    def project(c, carry):
        rows_f = resid_ref[:, cols(c)].astype(jnp.float32) * scale
        normed = jnp.concatenate(
            [rows_f[:, j * 128:(j + 1) * 128] * gain_f[pl.ds(c * (depth // 128) + j, 1), :]
             for j in range(depth // 128)], axis=-1).astype(jnp.bfloat16)
        for copy in w_copies(c):
            copy.wait()

        @pl.when(c + W_AHEAD < n_w)
        def _():
            for copy in w_copies(c + W_AHEAD):
                copy.start()

        @pl.when(c >= n_w // 2)
        def _():
            for i in range(per_step):
                for copy in in_copies((c - n_w // 2) * per_step + i):
                    copy.start()

        acc[...] += jnp.dot(normed, w_buf[c], preferred_element_type=jnp.float32)
        return carry

    with jax.named_scope('project'):
        lax.fori_loop(0, n_w, project, 0)

    def rotate(cols_f):
        values = cols_f.astype(jnp.bfloat16).astype(jnp.float32)
        turned = values * cos_ref[...] + pltpu.roll(values, head_dim // 2, 1) * sin_ref[...]
        return turned.astype(jnp.bfloat16).astype(jnp.float32)

    for j in range(group_size):
        q_rows[pl.ds(j, n_seqs, stride=group_size), :] = rotate(acc[:, j * head_dim:(j + 1) * head_dim])
    k_new[...] = rotate(acc[:, q_width:q_width + head_dim])
    v_new[...] = acc[:, q_width + head_dim:].astype(jnp.bfloat16).astype(jnp.float32)
    inv_sqrt = 1.0 / math.sqrt(head_dim)

    def attend(b, carry):
        for copy in in_copies(b):
            copy.wait()
        for i in range(SEQ_BLOCK):
            seq = b * SEQ_BLOCK + i
            pos = pos_ref[seq]
            base = pl.multiple_of(pos // 16 * 16, 16)
            hit = lax.broadcasted_iota(jnp.int32, (16, head_dim), 0) == pos - base
            for buf, new in ((k_buf, k_new), (v_buf, v_new)):
                old = buf[seq, pl.ds(base, 16), :].astype(jnp.float32)
                buf[seq, pl.ds(base, 16), :] = jnp.where(hit, new[pl.ds(seq, 1), :], old).astype(jnp.bfloat16)
        for copy in out_copies(b):
            copy.start()
        rows, probs = [], []
        for i in range(SEQ_BLOCK):
            seq = b * SEQ_BLOCK + i
            rows.append(pl.ds(pl.multiple_of(seq * group_size, group_size), group_size))
            query = q_rows[rows[i], :].astype(jnp.bfloat16)
            scores = lax.dot_general(query, k_buf[seq], (((1,), (1,)), ((), ())),
                                     preferred_element_type=jnp.float32) * inv_sqrt
            valid = lax.broadcasted_iota(jnp.int32, scores.shape, 1) <= pos_ref[seq]
            scores = jnp.where(valid, scores, -jnp.inf)
            exps = jnp.exp(scores - jnp.max(scores, axis=-1, keepdims=True))
            probs.append((exps / jnp.sum(exps, axis=-1, keepdims=True)).astype(jnp.bfloat16))
        for i in range(SEQ_BLOCK):
            o_rows[rows[i], :] = jnp.dot(probs[i], v_buf[b * SEQ_BLOCK + i], preferred_element_type=jnp.float32)
        return carry

    with jax.named_scope('attend'):
        lax.fori_loop(0, n_block, attend, 0)
    for j in range(group_size):
        attn_ref[:, j * head_dim:(j + 1) * head_dim] = (
            o_rows[pl.ds(j, n_seqs, stride=group_size), :].astype(jnp.bfloat16))
    for b in range(n_block):
        for copy in out_copies(b):
            copy.wait()


SEQ_BLOCK = 32
FRONT_DEPTH = 1024
W_AHEAD = 4


def layer_front(resid_in, positions, k_cache, v_cache, gain_attn, w_query, w_key, w_value):
    n_seqs, width = resid_in.shape
    cache_len, head_dim = k_cache.shape[1], k_cache.shape[3]
    q_width = w_query.shape[1]
    f32, bf16 = jnp.float32, jnp.bfloat16
    vmem = pl.BlockSpec(memory_space=pltpu.VMEM)
    hbm = pl.BlockSpec(memory_space=pl.ANY)
    dma = pltpu.SemaphoreType.DMA
    n_w, n_block = width // FRONT_DEPTH, n_seqs // SEQ_BLOCK
    flat = (n_seqs, cache_len, head_dim)
    attn_out, k_out, v_out = pl.pallas_call(
        front_kernel,
        out_shape=(jax.ShapeDtypeStruct((n_seqs, q_width), bf16),
                   jax.ShapeDtypeStruct(flat, bf16), jax.ShapeDtypeStruct(flat, bf16)),
        in_specs=[pl.BlockSpec(memory_space=pltpu.SMEM), hbm, vmem, vmem, vmem, hbm, hbm, hbm, hbm, hbm],
        out_specs=(vmem, hbm, hbm),
        scratch_shapes=[
            pltpu.VMEM((n_w, FRONT_DEPTH, q_width + 2 * head_dim), bf16),
            pltpu.VMEM((n_seqs, q_width + 2 * head_dim), f32),
            pltpu.VMEM(flat, bf16),
            pltpu.VMEM(flat, bf16),
            pltpu.VMEM((n_seqs * q_width // head_dim, head_dim), f32),
            pltpu.VMEM((n_seqs * q_width // head_dim, head_dim), f32),
            pltpu.VMEM((n_seqs, head_dim), f32),
            pltpu.VMEM((n_seqs, head_dim), f32),
            pltpu.VMEM((width // 128, 128), f32),
            pltpu.VMEM((n_seqs, head_dim), f32),
            pltpu.VMEM((n_seqs, head_dim), f32),
            pltpu.VMEM((n_seqs, width), bf16),
            dma(()),
            dma((3, n_w)),
            dma((2, n_block)),
            dma((2, n_block)),
        ],
        compiler_params=pltpu.CompilerParams(vmem_limit_bytes=55050240),
        name='layer_front',
    )(positions, resid_in, gain_attn.reshape(width // 128, 128), positions[None, :],
      rope_freqs(head_dim), w_query, w_key, w_value,
      k_cache.reshape(flat), v_cache.reshape(flat))
    return attn_out, k_out.reshape(k_cache.shape), v_out.reshape(v_cache.shape)


N_CHUNK = 16
N_SLOT = 11
T_ROWS = 1280
MESH = pl.DeviceIdType.MESH


def tail_kernel(attn_ref, resid_hbm, gain_ref, w_out_hbm, gate_t_hbm, up_t_hbm, w_down_hbm, out_ref,
                part, from_core, from_1, from_2, gathered, mid, sq_sum, resid_own, gain_f,
                gate_acc, up_acc, gate_acc_t, up_acc_t, turned, hidden, ring,
                resid_sem, out_sem, ring_sem, rs_send, rs_recv, ag_send, ag_recv):
    n_chunk, chunk = N_CHUNK, part.shape[-1]
    half = chunk // 2
    rows = mid.shape[1]
    me = lax.axis_index('tp')
    k = me % 2
    x = (me // 2) % 2
    y = me // 4
    nk, nx, ny = 1 - k, 1 - x, 1 - y
    core_nbr = {'tp': me + 1 - 2 * k}
    x_nbr = {'tp': me + 2 - 4 * x}
    y_nbr = {'tp': me + 4 - 8 * y}

    def cols(c):
        return pl.ds(pl.multiple_of(c * chunk, chunk), chunk)

    depth_out = w_out_hbm.shape[0]
    first_mlp = n_chunk // 2
    first_down = first_mlp + 2 * n_chunk

    def out_slot(c):
        return c // 2, pl.ds(pl.multiple_of((c % 2) * depth_out, depth_out), depth_out)

    def out_copy(c):
        slot, span = out_slot(c)
        return pltpu.make_async_copy(w_out_hbm.at[:, cols(c)], ring.at[slot, span], out_sem.at[c])

    def ring_copy(src, c, j):
        slot = j % N_SLOT
        return pltpu.make_async_copy(src.at[:, cols(c)], ring.at[slot], ring_sem.at[slot])

    def gate_copy(c):
        return ring_copy(gate_t_hbm, c, first_mlp + 2 * c)

    def up_copy(c):
        return ring_copy(up_t_hbm, c, first_mlp + 2 * c + 1)

    def down_copy(c):
        return ring_copy(w_down_hbm, c, first_down + c)

    def start_load(j):
        m = j - first_mlp

        @pl.when(j < first_down)
        def _():
            @pl.when(m % 2 == 0)
            def _():
                gate_copy(m // 2).start()

            @pl.when(m % 2 == 1)
            def _():
                up_copy(m // 2).start()

        @pl.when(jnp.logical_and(j >= first_down, j < first_down + n_chunk))
        def _():
            down_copy(j - first_down).start()

    row0 = pl.multiple_of(64 * k + 32 * x + 16 * y, 16)
    resid_copy = pltpu.make_async_copy(resid_hbm.at[pl.ds(row0, rows)], resid_own, resid_sem)
    resid_copy.start()
    for c in range(OUT_AHEAD):
        out_copy(c).start()

    barrier = pltpu.get_barrier_semaphore()
    for nbr in (core_nbr, x_nbr, y_nbr):
        pl.semaphore_signal(barrier, inc=1, device_id=nbr, device_id_type=MESH)

    def remote(src, dst, sems, ch, c, nbr):
        return pltpu.make_async_remote_copy(src_ref=src, dst_ref=dst, send_sem=sems[0].at[c],
                                            recv_sem=sems[1].at[ch, c], device_id=nbr, device_id_type=MESH)

    def wait_bytes(ref, sem):
        pltpu.make_async_copy(ref, ref, sem).wait()

    def wait_sent(sems, c):
        wait_bytes(mid.at[pl.ds(0, 7)], sems[0].at[c])

    rs = (rs_send, rs_recv)
    ag = (ag_send, ag_recv)
    left, right = pl.ds(0, half), pl.ds(half, half)

    def rs_core(c):
        return remote(part.at[c, nk], from_core.at[c], rs, 0, c, core_nbr)

    def rs_x1(c):
        return remote(part.at[c, k, nx, :, :, left], from_1.at[c, 0], rs, 1, c, x_nbr)

    def rs_y1(c):
        return remote(part.at[c, k, :, ny, :, right], from_1.at[c, 1], rs, 1, c, y_nbr)

    def rs_y2(c):
        return remote(part.at[c, k, x, ny, :, left], from_2.at[c, 0], rs, 2, c, y_nbr)

    def rs_x2(c):
        return remote(part.at[c, k, nx, y, :, right], from_2.at[c, 1], rs, 2, c, x_nbr)

    def ag_x(c):
        blk = gathered.at[c, k, x, y]
        return remote(blk, blk, ag, 0, c, x_nbr)

    def ag_y(c):
        blk = gathered.at[c, k, x, y]
        return remote(blk, blk, ag, 0, c, y_nbr)

    def ag_fwd_y(c):
        blk = gathered.at[c, k, nx, y, :, right]
        return remote(blk, blk, ag, 1, c, y_nbr)

    def ag_fwd_x(c):
        blk = gathered.at[c, k, x, ny, :, left]
        return remote(blk, blk, ag, 1, c, x_nbr)

    def ag_core(c):
        blk = gathered.at[c, k]
        return remote(blk, blk, ag, 2, c, core_nbr)

    def stage(s, lag, fn):
        c = s - lag

        @pl.when(jnp.logical_and(c >= 0, c < n_chunk))
        def _():
            with jax.named_scope(fn.__name__):
                fn(c)

    def rs_stage1(c):
        rs_core(c).wait_recv()
        part[c, k] = part[c, k] + from_core[c]
        rs_x1(c).start()
        rs_y1(c).start()

    def rs_stage2(c):
        wait_bytes(from_1.at[c], rs_recv.at[1, c])
        part[c, k, x, :, :, left] = part[c, k, x, :, :, left] + from_1[c, 0]
        part[c, k, :, y, :, right] = part[c, k, :, y, :, right] + from_1[c, 1]
        rs_y2(c).start()
        rs_x2(c).start()

    def rs_stage3(c):
        wait_bytes(from_2.at[c], rs_recv.at[2, c])
        total = jnp.concatenate([part[c, k, x, y, :, left] + from_2[c, 0],
                                 part[c, k, x, y, :, right] + from_2[c, 1]], axis=-1)
        wait_sent(rs, c)
        return total

    def ag_stage1(c):
        wait_bytes(from_1.at[c], ag_recv.at[0, c])
        ag_fwd_y(c).start()
        ag_fwd_x(c).start()

    def ag_stage2(c):
        wait_bytes(from_2.at[c], ag_recv.at[1, c])
        ag_core(c).start()

    def ag_stage3(c):
        ag_core(c).wait_recv()
        block = gathered[c].reshape(8 * rows, chunk)
        wait_sent(ag, c)
        return block

    gain_f[...] = gain_ref[...].astype(jnp.float32)
    sq_sum[...] = jnp.zeros_like(sq_sum)
    gate_acc[...] = jnp.zeros_like(gate_acc)
    up_acc[...] = jnp.zeros_like(up_acc)
    gate_acc_t[...] = jnp.zeros_like(gate_acc_t)
    up_acc_t[...] = jnp.zeros_like(up_acc_t)
    resid_copy.wait()
    with jax.named_scope('entry_barrier'):
        pl.semaphore_wait(barrier, 3)

    def proj(c):
        out_copy(c).wait()
        slot, span = out_slot(c)
        res = jnp.dot(attn_ref[...], ring[slot, span], preferred_element_type=jnp.float32)
        part[c] = res.reshape(part.shape[1:])
        rs_core(c).start()

        @pl.when(c + OUT_AHEAD < n_chunk)
        def _():
            out_copy(c + OUT_AHEAD).start()

        @pl.when(first_mlp + c < N_SLOT)
        def _():
            start_load(first_mlp + c)

        @pl.when(c % 2 == 1)
        def _():
            start_load(c // 2 + N_SLOT)

    def finish_mid(c):
        total = rs_stage3(c)
        x1 = (resid_own[:, cols(c)].astype(jnp.float32) + total).astype(jnp.bfloat16).astype(jnp.float32)
        mid[c] = x1
        sq_sum[...] += x1 * x1

    def rs_body(s, carry):
        stage(s, 0, proj)
        stage(s, RS1_LAG[0], rs_stage1)
        stage(s, RS1_LAG[1], rs_stage2)
        stage(s, RS1_LAG[2], finish_mid)
        return carry

    with jax.named_scope('phase_rs1'):
        lax.fori_loop(0, n_chunk + RS1_LAG[2], rs_body, 0)

    mean_sq = jnp.sum(sq_sum[...], axis=-1, keepdims=True) * (1.0 / (n_chunk * chunk))
    scale = lax.rsqrt(mean_sq + EPS)

    def send_normed(c):
        gain = jnp.concatenate([gain_f[pl.ds(c * (chunk // 128) + j, 1), :] for j in range(chunk // 128)], axis=-1)
        normed = (mid[c] * scale * gain).astype(jnp.bfloat16)
        gathered[c, k, x, y] = normed.astype(jnp.float32)
        ag_x(c).start()
        ag_y(c).start()

    def gate_up(c):
        block = ag_stage3(c).astype(jnp.bfloat16)
        gate_copy(c).wait()
        up_copy(c).wait()
        first = first_mlp + 2 * c
        accs = ((gate_acc, gate_acc_t), (up_acc, up_acc_t))
        for i, (acc, acc_t) in enumerate(accs):
            slot = (first + i) % N_SLOT
            turned[i] = ring[slot, pl.ds(T_ROWS, acc_t.shape[1])].T
            acc[...] += lax.dot_general(ring[slot, pl.ds(0, T_ROWS)], block, (((1,), (1,)), ((), ())),
                                        preferred_element_type=jnp.float32)
        for i, (acc, acc_t) in enumerate(accs):
            acc_t[...] += jnp.dot(block, turned[i], preferred_element_type=jnp.float32)
        for i in range(2):
            start_load(first + i + N_SLOT)

    def ag_body(s, carry):
        stage(s, 0, send_normed)
        stage(s, AG1_LAG[0], ag_stage1)
        stage(s, AG1_LAG[1], ag_stage2)
        stage(s, AG1_LAG[2], gate_up)
        return carry

    with jax.named_scope('phase_ag1'):
        lax.fori_loop(0, n_chunk + AG1_LAG[2], ag_body, 0)

    def act(gate, up):
        gate = gate.astype(jnp.bfloat16).astype(jnp.float32)
        up = up.astype(jnp.bfloat16).astype(jnp.float32)
        return jax.nn.silu(gate) * up

    for lo in range(0, T_ROWS, 128):
        span = slice(lo, lo + 128)
        hidden[:, span] = act(gate_acc[span, :], up_acc[span, :]).T.astype(jnp.bfloat16)
    hidden[:, T_ROWS:] = act(gate_acc_t[...], up_acc_t[...]).astype(jnp.bfloat16)

    def down(c):
        down_copy(c).wait()
        j = first_down + c
        res = jnp.dot(hidden[...], ring[j % N_SLOT], preferred_element_type=jnp.float32)
        part[c] = res.reshape(part.shape[1:])
        rs_core(c).start()
        start_load(j + N_SLOT)

    def finish_out(c):
        total = rs_stage3(c)
        gathered[c, k, x, y] = (mid[c] + total).astype(jnp.bfloat16).astype(jnp.float32)
        ag_x(c).start()
        ag_y(c).start()

    def store_out(c):
        out_ref[:, cols(c)] = ag_stage3(c).astype(jnp.bfloat16)

    base = RS2_LAG[2]

    def down_body(s, carry):
        stage(s, 0, down)
        stage(s, RS2_LAG[0], rs_stage1)
        stage(s, RS2_LAG[1], rs_stage2)
        stage(s, base, finish_out)
        stage(s, base + AG2_LAG[0], ag_stage1)
        stage(s, base + AG2_LAG[1], ag_stage2)
        stage(s, base + AG2_LAG[2], store_out)
        return carry

    with jax.named_scope('phase_ar2'):
        lax.fori_loop(0, n_chunk + base + AG2_LAG[2], down_body, 0)


RS1_LAG = (2, 6, 10)
AG1_LAG = (2, 4, 5)
RS2_LAG = (2, 5, 8)
AG2_LAG = (2, 4, 5)
OUT_AHEAD = 5


def layer_tail(attn_out, resid_in, gain_mlp, w_out, w_gate, w_up, w_down):
    n_rows, width = resid_in.shape
    ffn = w_gate.shape[1]
    chunk = width // N_CHUNK
    half = chunk // 2
    rows = n_rows // 8
    f32, bf16 = jnp.float32, jnp.bfloat16
    vmem = pl.BlockSpec(memory_space=pltpu.VMEM)
    hbm = pl.BlockSpec(memory_space=pl.ANY)
    dma = pltpu.SemaphoreType.DMA
    return pl.pallas_call(
        tail_kernel,
        out_shape=jax.ShapeDtypeStruct((n_rows, width), bf16),
        in_specs=[vmem, hbm, vmem, hbm, hbm, hbm, hbm],
        out_specs=vmem,
        scratch_shapes=[
            pltpu.VMEM((N_CHUNK, 2, 2, 2, rows, chunk), f32),
            pltpu.VMEM((N_CHUNK, 2, 2, rows, chunk), f32),
            pltpu.VMEM((N_CHUNK, 2, 2, rows, half), f32),
            pltpu.VMEM((N_CHUNK, 2, rows, half), f32),
            pltpu.VMEM((N_CHUNK, 2, 2, 2, rows, chunk), f32),
            pltpu.VMEM((N_CHUNK, rows, chunk), f32),
            pltpu.VMEM((rows, chunk), f32),
            pltpu.VMEM((rows, width), bf16),
            pltpu.VMEM((width // 128, 128), f32),
            pltpu.VMEM((T_ROWS, n_rows), f32),
            pltpu.VMEM((T_ROWS, n_rows), f32),
            pltpu.VMEM((n_rows, ffn - T_ROWS), f32),
            pltpu.VMEM((n_rows, ffn - T_ROWS), f32),
            pltpu.VMEM((2, chunk, ffn - T_ROWS), bf16),
            pltpu.VMEM((n_rows, ffn), bf16),
            pltpu.VMEM((N_SLOT, ffn, chunk), bf16),
            dma(()),
            dma((N_CHUNK,)),
            dma((N_SLOT,)),
            dma((N_CHUNK,)),
            dma((3, N_CHUNK)),
            dma((N_CHUNK,)),
            dma((3, N_CHUNK)),
        ],
        compiler_params=pltpu.CompilerParams(collective_id=0, has_side_effects=True,
                                             vmem_limit_bytes=53477376),
        name='layer_tail',
    )(attn_out, resid_in, gain_mlp.reshape(width // 128, 128), w_out, w_gate.T, w_up.T, w_down)


def solution(mesh):
    def layer_local(resid_in, positions, k_cache, v_cache, gain_attn, w_query, w_key, w_value,
                    w_out, gain_mlp, w_gate, w_up, w_down):
        attn_out, k_full, v_full = layer_front(resid_in, positions, k_cache, v_cache,
                                               gain_attn, w_query, w_key, w_value)
        resid_out = layer_tail(attn_out, resid_in, gain_mlp, w_out, w_gate, w_up, w_down)
        return resid_out, k_full, v_full

    row_spec = P('dp', None)
    cache_spec = P('dp', None, 'tp', None)
    col_spec = P(None, 'tp')
    split_rows = P('tp', None)
    return jax.shard_map(layer_local, mesh=mesh,
                         in_specs=(row_spec, P('dp'), cache_spec, cache_spec, P(), col_spec, col_spec,
                                   col_spec, split_rows, P(), col_spec, col_spec, split_rows),
                         out_specs=(row_spec, cache_spec, cache_spec), check_vma=False)
```

```python
import math
import jax
import jax.numpy as jnp
from jax import lax
from jax.experimental import pallas as pl
from jax.experimental.pallas import tpu as pltpu
from jax.sharding import PartitionSpec as P

EPS = 1e-5
ROPE_THETA = 500000.0
ROPE_FACTOR = 8.0
LOW_FACTOR = 1.0
HIGH_FACTOR = 4.0
ORIG_CTX = 8192.0


def rope_freqs(head_dim):
    half_dim = head_dim // 2
    exponents = (jnp.arange(head_dim, dtype=jnp.int32) % half_dim).astype(jnp.float32) * (2.0 / head_dim)
    inv_freq = 1.0 / jnp.power(ROPE_THETA, exponents)
    wavelen = (2.0 * math.pi) / inv_freq
    smooth = (ORIG_CTX / wavelen - LOW_FACTOR) / (HIGH_FACTOR - LOW_FACTOR)
    blended = (1.0 - smooth) * inv_freq / ROPE_FACTOR + smooth * inv_freq
    inv_freq = jnp.where(wavelen < ORIG_CTX / HIGH_FACTOR, inv_freq,
                         jnp.where(wavelen > ORIG_CTX / LOW_FACTOR, inv_freq / ROPE_FACTOR, blended))
    return inv_freq[None, :]


def front_kernel(pos_ref, resid_hbm, gain_ref, pos_row_ref, freq_ref, w_query_hbm, w_key_hbm, w_value_hbm,
                 k_in_hbm, v_in_hbm, attn_ref, k_out_hbm, v_out_hbm,
                 w_buf, acc, k_buf, v_buf, q_rows, o_rows, k_new, v_new, gain_f, cos_ref, sin_ref, resid_ref,
                 resid_sem, w_sem, cache_sem, out_sem):
    n_seqs, width = resid_ref.shape
    depth, q_width = w_buf.shape[1], w_query_hbm.shape[1]
    head_dim = k_new.shape[1]
    group_size = q_width // head_dim
    n_block = n_seqs // SEQ_BLOCK

    def w_copies(c):
        span = pl.ds(pl.multiple_of(c * depth, depth), depth)
        copies = []
        for i, (src, lo, size) in enumerate(((w_query_hbm, 0, q_width), (w_key_hbm, q_width, head_dim),
                                             (w_value_hbm, q_width + head_dim, head_dim))):
            copies.append(pltpu.make_async_copy(src.at[span], w_buf.at[c, :, pl.ds(lo, size)], w_sem.at[i, c]))
        return copies

    def block(b):
        return pl.ds(pl.multiple_of(b * SEQ_BLOCK, SEQ_BLOCK), SEQ_BLOCK)

    def in_copies(b):
        return (pltpu.make_async_copy(k_in_hbm.at[block(b)], k_buf.at[block(b)], cache_sem.at[0, b]),
                pltpu.make_async_copy(v_in_hbm.at[block(b)], v_buf.at[block(b)], cache_sem.at[1, b]))

    def out_copies(b):
        return (pltpu.make_async_copy(k_buf.at[block(b)], k_out_hbm.at[block(b)], out_sem.at[0, b]),
                pltpu.make_async_copy(v_buf.at[block(b)], v_out_hbm.at[block(b)], out_sem.at[1, b]))

    n_w = width // depth
    resid_copy = pltpu.make_async_copy(resid_hbm, resid_ref, resid_sem)
    resid_copy.start()
    for copy in w_copies(0):
        copy.start()
    gain_f[...] = gain_ref[...].astype(jnp.float32)

    def cols(c):
        return pl.ds(pl.multiple_of(c * depth, depth), depth)

    def add_squares(c, total):
        part = resid_ref[:, cols(c)].astype(jnp.float32)
        part = part * part
        for j in range(depth // 128):
            total = total + part[:, j * 128:(j + 1) * 128]
        return total

    acc[...] = jnp.zeros_like(acc)
    angles = (jnp.broadcast_to(pos_row_ref[...].astype(jnp.float32), (n_seqs, n_seqs)).T[:, :1]
              * freq_ref[...])
    cos_f = jnp.cos(angles)
    sin_f = jnp.sin(angles)
    sin_f = jnp.where(lax.broadcasted_iota(jnp.int32, sin_f.shape, 1) < head_dim // 2, -sin_f, sin_f)
    cos_ref[...] = cos_f
    sin_ref[...] = sin_f
    resid_copy.wait()
    for c in range(1, W_AHEAD):
        for copy in w_copies(c):
            copy.start()
    squares = lax.fori_loop(0, n_w, add_squares, jnp.zeros((n_seqs, 128), jnp.float32))
    scale = lax.rsqrt(jnp.sum(squares, axis=-1, keepdims=True) * (1.0 / width) + EPS)
    per_step = n_block // (n_w // 2)

    def project(c, carry):
        rows_f = resid_ref[:, cols(c)].astype(jnp.float32) * scale
        normed = jnp.concatenate(
            [rows_f[:, j * 128:(j + 1) * 128] * gain_f[pl.ds(c * (depth // 128) + j, 1), :]
             for j in range(depth // 128)], axis=-1).astype(jnp.bfloat16)
        for copy in w_copies(c):
            copy.wait()

        @pl.when(c + W_AHEAD < n_w)
        def _():
            for copy in w_copies(c + W_AHEAD):
                copy.start()

        @pl.when(c >= n_w // 2)
        def _():
            for i in range(per_step):
                for copy in in_copies((c - n_w // 2) * per_step + i):
                    copy.start()

        acc[...] += jnp.dot(normed, w_buf[c], preferred_element_type=jnp.float32)
        return carry

    lax.fori_loop(0, n_w, project, 0)

    def rotate(cols_f):
        values = cols_f.astype(jnp.bfloat16).astype(jnp.float32)
        turned = values * cos_ref[...] + pltpu.roll(values, head_dim // 2, 1) * sin_ref[...]
        return turned.astype(jnp.bfloat16).astype(jnp.float32)

    for j in range(group_size):
        q_rows[pl.ds(j, n_seqs, stride=group_size), :] = rotate(acc[:, j * head_dim:(j + 1) * head_dim])
    k_new[...] = rotate(acc[:, q_width:q_width + head_dim])
    v_new[...] = acc[:, q_width + head_dim:].astype(jnp.bfloat16).astype(jnp.float32)
    inv_sqrt = 1.0 / math.sqrt(head_dim)

    def attend(b, carry):
        for copy in in_copies(b):
            copy.wait()
        for i in range(SEQ_BLOCK):
            seq = b * SEQ_BLOCK + i
            pos = pos_ref[seq]
            base = pl.multiple_of(pos // 16 * 16, 16)
            hit = lax.broadcasted_iota(jnp.int32, (16, head_dim), 0) == pos - base
            for buf, new in ((k_buf, k_new), (v_buf, v_new)):
                old = buf[seq, pl.ds(base, 16), :].astype(jnp.float32)
                buf[seq, pl.ds(base, 16), :] = jnp.where(hit, new[pl.ds(seq, 1), :], old).astype(jnp.bfloat16)
        for copy in out_copies(b):
            copy.start()
        rows, probs = [], []
        for i in range(SEQ_BLOCK):
            seq = b * SEQ_BLOCK + i
            rows.append(pl.ds(pl.multiple_of(seq * group_size, group_size), group_size))
            query = q_rows[rows[i], :].astype(jnp.bfloat16)
            scores = lax.dot_general(query, k_buf[seq], (((1,), (1,)), ((), ())),
                                     preferred_element_type=jnp.float32) * inv_sqrt
            valid = lax.broadcasted_iota(jnp.int32, scores.shape, 1) <= pos_ref[seq]
            scores = jnp.where(valid, scores, -jnp.inf)
            exps = jnp.exp(scores - jnp.max(scores, axis=-1, keepdims=True))
            probs.append((exps / jnp.sum(exps, axis=-1, keepdims=True)).astype(jnp.bfloat16))
        for i in range(SEQ_BLOCK):
            o_rows[rows[i], :] = jnp.dot(probs[i], v_buf[b * SEQ_BLOCK + i], preferred_element_type=jnp.float32)
        return carry

    lax.fori_loop(0, n_block, attend, 0)
    for j in range(group_size):
        attn_ref[:, j * head_dim:(j + 1) * head_dim] = (
            o_rows[pl.ds(j, n_seqs, stride=group_size), :].astype(jnp.bfloat16))
    for b in range(n_block):
        for copy in out_copies(b):
            copy.wait()


SEQ_BLOCK = 32
FRONT_DEPTH = 2048
W_AHEAD = 2


def layer_front(resid_in, positions, k_cache, v_cache, gain_attn, w_query, w_key, w_value):
    n_seqs, width = resid_in.shape
    cache_len, head_dim = k_cache.shape[1], k_cache.shape[3]
    q_width = w_query.shape[1]
    f32, bf16 = jnp.float32, jnp.bfloat16
    vmem = pl.BlockSpec(memory_space=pltpu.VMEM)
    hbm = pl.BlockSpec(memory_space=pl.ANY)
    dma = pltpu.SemaphoreType.DMA
    n_w, n_block = width // FRONT_DEPTH, n_seqs // SEQ_BLOCK
    flat = (n_seqs, cache_len, head_dim)
    attn_out, k_out, v_out = pl.pallas_call(
        front_kernel,
        out_shape=(jax.ShapeDtypeStruct((n_seqs, q_width), bf16),
                   jax.ShapeDtypeStruct(flat, bf16), jax.ShapeDtypeStruct(flat, bf16)),
        in_specs=[pl.BlockSpec(memory_space=pltpu.SMEM), hbm, vmem, vmem, vmem, hbm, hbm, hbm, hbm, hbm],
        out_specs=(vmem, hbm, hbm),
        scratch_shapes=[
            pltpu.VMEM((n_w, FRONT_DEPTH, q_width + 2 * head_dim), bf16),
            pltpu.VMEM((n_seqs, q_width + 2 * head_dim), f32),
            pltpu.VMEM(flat, bf16),
            pltpu.VMEM(flat, bf16),
            pltpu.VMEM((n_seqs * q_width // head_dim, head_dim), f32),
            pltpu.VMEM((n_seqs * q_width // head_dim, head_dim), f32),
            pltpu.VMEM((n_seqs, head_dim), f32),
            pltpu.VMEM((n_seqs, head_dim), f32),
            pltpu.VMEM((width // 128, 128), f32),
            pltpu.VMEM((n_seqs, head_dim), f32),
            pltpu.VMEM((n_seqs, head_dim), f32),
            pltpu.VMEM((n_seqs, width), bf16),
            dma(()),
            dma((3, n_w)),
            dma((2, n_block)),
            dma((2, n_block)),
        ],
        compiler_params=pltpu.CompilerParams(vmem_limit_bytes=55050240),
        name='layer_front',
    )(positions, resid_in, pltpu.with_memory_space_constraint(gain_attn.reshape(width // 128, 128), pltpu.HBM),
      pltpu.with_memory_space_constraint(positions[None, :], pltpu.HBM),
      rope_freqs(head_dim), w_query, w_key, w_value,
      k_cache.reshape(flat), v_cache.reshape(flat))
    return attn_out, k_out.reshape(k_cache.shape), v_out.reshape(v_cache.shape)


N_CHUNK = 16
N_SLOT = 11
T_ROWS = 1024
MESH = pl.DeviceIdType.MESH


def tail_kernel(attn_ref, resid_hbm, gain_ref, w_out_hbm, gate_t_hbm, up_t_hbm, w_down_hbm, out_ref,
                part, from_core, from_1, from_2, gathered, mid, sq_sum, resid_own, gain_f,
                gate_acc, up_acc, gate_acc_t, up_acc_t, turned, hidden, ring,
                resid_sem, out_sem, ring_sem, rs_send, rs_recv, ag_send, ag_recv):
    n_chunk, chunk = N_CHUNK, part.shape[-1]
    half = chunk // 2
    rows = mid.shape[1]
    me = lax.axis_index('tp')
    k = me % 2
    x = (me // 2) % 2
    y = me // 4
    nk, nx, ny = 1 - k, 1 - x, 1 - y
    core_nbr = {'tp': me + 1 - 2 * k}
    x_nbr = {'tp': me + 2 - 4 * x}
    y_nbr = {'tp': me + 4 - 8 * y}

    def cols(c):
        return pl.ds(pl.multiple_of(c * chunk, chunk), chunk)

    depth_out = w_out_hbm.shape[0]
    first_mlp = n_chunk // 2
    first_down = first_mlp + 2 * n_chunk

    def out_slot(c):
        return c // 2, pl.ds(pl.multiple_of((c % 2) * depth_out, depth_out), depth_out)

    def out_copy(c):
        slot, span = out_slot(c)
        return pltpu.make_async_copy(w_out_hbm.at[:, cols(c)], ring.at[slot, span], out_sem.at[c])

    def ring_copy(src, c, j):
        slot = j % N_SLOT
        return pltpu.make_async_copy(src.at[:, cols(c)], ring.at[slot], ring_sem.at[slot])

    def gate_copy(c):
        return ring_copy(gate_t_hbm, c, first_mlp + 2 * c)

    def up_copy(c):
        return ring_copy(up_t_hbm, c, first_mlp + 2 * c + 1)

    def down_copy(c):
        return ring_copy(w_down_hbm, c, first_down + c)

    def start_load(j):
        m = j - first_mlp

        @pl.when(j < first_down)
        def _():
            @pl.when(m % 2 == 0)
            def _():
                gate_copy(m // 2).start()

            @pl.when(m % 2 == 1)
            def _():
                up_copy(m // 2).start()

        @pl.when(jnp.logical_and(j >= first_down, j < first_down + n_chunk))
        def _():
            down_copy(j - first_down).start()

    row0 = pl.multiple_of(64 * k + 32 * x + 16 * y, 16)
    resid_copy = pltpu.make_async_copy(resid_hbm.at[pl.ds(row0, rows)], resid_own, resid_sem)
    out_copy(0).start()

    barrier = pltpu.get_barrier_semaphore()
    for nbr in (core_nbr, x_nbr, y_nbr):
        pl.semaphore_signal(barrier, inc=1, device_id=nbr, device_id_type=MESH)

    def remote(src, dst, sems, ch, c, nbr):
        return pltpu.make_async_remote_copy(src_ref=src, dst_ref=dst, send_sem=sems[0].at[c],
                                            recv_sem=sems[1].at[ch, c], device_id=nbr, device_id_type=MESH)

    def wait_bytes(ref, sem):
        pltpu.make_async_copy(ref, ref, sem).wait()

    def wait_sent(sems, c):
        wait_bytes(mid.at[pl.ds(0, 7)], sems[0].at[c])

    rs = (rs_send, rs_recv)
    ag = (ag_send, ag_recv)
    left, right = pl.ds(0, half), pl.ds(half, half)

    def rs_core(c):
        return remote(part.at[c, nk], from_core.at[c], rs, 0, c, core_nbr)

    def rs_x1(c):
        return remote(part.at[c, k, nx, :, :, left], from_1.at[c, 0], rs, 1, c, x_nbr)

    def rs_y1(c):
        return remote(part.at[c, k, :, ny, :, right], from_1.at[c, 1], rs, 1, c, y_nbr)

    def rs_y2(c):
        return remote(part.at[c, k, x, ny, :, left], from_2.at[c, 0], rs, 2, c, y_nbr)

    def rs_x2(c):
        return remote(part.at[c, k, nx, y, :, right], from_2.at[c, 1], rs, 2, c, x_nbr)

    def ag_x(c):
        blk = gathered.at[c, k, x, y]
        return remote(blk, blk, ag, 0, c, x_nbr)

    def ag_y(c):
        blk = gathered.at[c, k, x, y]
        return remote(blk, blk, ag, 0, c, y_nbr)

    def ag_fwd_y(c):
        blk = gathered.at[c, k, nx, y, :, right]
        return remote(blk, blk, ag, 1, c, y_nbr)

    def ag_fwd_x(c):
        blk = gathered.at[c, k, x, ny, :, left]
        return remote(blk, blk, ag, 1, c, x_nbr)

    def ag_core(c):
        blk = gathered.at[c, k]
        return remote(blk, blk, ag, 2, c, core_nbr)

    def stage(s, lag, fn):
        c = s - lag

        @pl.when(jnp.logical_and(c >= 0, c < n_chunk))
        def _():
            fn(c)

    def rs_stage1(c):
        rs_core(c).wait_recv()
        part[c, k] = part[c, k] + from_core[c]
        rs_x1(c).start()
        rs_y1(c).start()

    def rs_stage2(c):
        wait_bytes(from_1.at[c], rs_recv.at[1, c])
        part[c, k, x, :, :, left] = part[c, k, x, :, :, left] + from_1[c, 0]
        part[c, k, :, y, :, right] = part[c, k, :, y, :, right] + from_1[c, 1]
        rs_y2(c).start()
        rs_x2(c).start()

    def rs_stage3(c):
        wait_bytes(from_2.at[c], rs_recv.at[2, c])
        total = jnp.concatenate([part[c, k, x, y, :, left] + from_2[c, 0],
                                 part[c, k, x, y, :, right] + from_2[c, 1]], axis=-1)
        wait_sent(rs, c)
        return total

    def ag_stage1(c):
        wait_bytes(from_1.at[c], ag_recv.at[0, c])
        ag_fwd_y(c).start()
        ag_fwd_x(c).start()

    def ag_stage2(c):
        wait_bytes(from_2.at[c], ag_recv.at[1, c])
        ag_core(c).start()

    def ag_stage3(c):
        ag_core(c).wait_recv()
        block = gathered[c].reshape(8 * rows, chunk)
        wait_sent(ag, c)
        return block

    gain_f[...] = gain_ref[...].astype(jnp.float32)
    sq_sum[...] = jnp.zeros_like(sq_sum)
    gate_acc[...] = jnp.zeros_like(gate_acc)
    up_acc[...] = jnp.zeros_like(up_acc)
    gate_acc_t[...] = jnp.zeros_like(gate_acc_t)
    up_acc_t[...] = jnp.zeros_like(up_acc_t)
    for c in range(1, OUT_AHEAD):
        out_copy(c).start()
    resid_copy.start()
    pl.semaphore_wait(barrier, 3)

    def proj(c):
        out_copy(c).wait()
        slot, span = out_slot(c)
        res = jnp.dot(attn_ref[...], ring[slot, span], preferred_element_type=jnp.float32)
        part[c] = res.reshape(part.shape[1:])
        rs_core(c).start()

        @pl.when(c + OUT_AHEAD < n_chunk)
        def _():
            out_copy(c + OUT_AHEAD).start()

        ahead = first_mlp + c - LOAD_LAG

        @pl.when(jnp.logical_and(c >= LOAD_LAG, ahead < N_SLOT))
        def _():
            start_load(ahead)

        @pl.when(c % 2 == 1)
        def _():
            start_load(c // 2 + N_SLOT)

    def finish_mid(c):
        @pl.when(c == 0)
        def _():
            resid_copy.wait()

        total = rs_stage3(c)
        x1 = (resid_own[:, cols(c)].astype(jnp.float32) + total).astype(jnp.bfloat16).astype(jnp.float32)
        mid[c] = x1
        sq_sum[...] += x1 * x1

    def rs_body(s, carry):
        stage(s, 0, proj)
        stage(s, RS1_LAG[0], rs_stage1)
        stage(s, RS1_LAG[1], rs_stage2)
        stage(s, RS1_LAG[2], finish_mid)
        return carry

    lax.fori_loop(0, n_chunk + RS1_LAG[2], rs_body, 0)

    mean_sq = jnp.sum(sq_sum[...], axis=-1, keepdims=True) * (1.0 / (n_chunk * chunk))
    scale = lax.rsqrt(mean_sq + EPS)

    def send_normed(c):
        gain = jnp.concatenate([gain_f[pl.ds(c * (chunk // 128) + j, 1), :] for j in range(chunk // 128)], axis=-1)
        normed = (mid[c] * scale * gain).astype(jnp.bfloat16)
        gathered[c, k, x, y] = normed.astype(jnp.float32)
        ag_x(c).start()
        ag_y(c).start()

    def gate_up(c):
        block = ag_stage3(c).astype(jnp.bfloat16)
        gate_copy(c).wait()
        up_copy(c).wait()
        first = first_mlp + 2 * c
        accs = ((gate_acc, gate_acc_t), (up_acc, up_acc_t))
        for i, (acc, acc_t) in enumerate(accs):
            slot = (first + i) % N_SLOT
            turned[i] = ring[slot, pl.ds(T_ROWS, acc_t.shape[1])].T
            acc[...] += lax.dot_general(ring[slot, pl.ds(0, T_ROWS)], block, (((1,), (1,)), ((), ())),
                                        preferred_element_type=jnp.float32)
        for i, (acc, acc_t) in enumerate(accs):
            acc_t[...] += jnp.dot(block, turned[i], preferred_element_type=jnp.float32)
        for i in range(2):
            start_load(first + i + N_SLOT)

    def ag_body(s, carry):
        stage(s, 0, send_normed)
        stage(s, AG1_LAG[0], ag_stage1)
        stage(s, AG1_LAG[1], ag_stage2)
        stage(s, AG1_LAG[2], gate_up)
        return carry

    lax.fori_loop(0, n_chunk + AG1_LAG[2], ag_body, 0)

    def act(gate, up):
        gate = gate.astype(jnp.bfloat16).astype(jnp.float32)
        up = up.astype(jnp.bfloat16).astype(jnp.float32)
        return jax.nn.silu(gate) * up

    for lo in range(0, T_ROWS, 128):
        span = slice(lo, lo + 128)
        hidden[:, span] = act(gate_acc[span, :], up_acc[span, :]).T.astype(jnp.bfloat16)
    hidden[:, T_ROWS:] = act(gate_acc_t[...], up_acc_t[...]).astype(jnp.bfloat16)

    def down(c):
        down_copy(c).wait()
        j = first_down + c
        res = jnp.dot(hidden[...], ring[j % N_SLOT], preferred_element_type=jnp.float32)
        part[c] = res.reshape(part.shape[1:])
        rs_core(c).start()
        start_load(j + N_SLOT)

    def finish_out(c):
        total = rs_stage3(c)
        gathered[c, k, x, y] = (mid[c] + total).astype(jnp.bfloat16).astype(jnp.float32)
        ag_x(c).start()
        ag_y(c).start()

    def store_out(c):
        out_ref[:, cols(c)] = ag_stage3(c).astype(jnp.bfloat16)

    base = RS2_LAG[2]

    def down_body(s, carry):
        stage(s, 0, down)
        stage(s, RS2_LAG[0], rs_stage1)
        stage(s, RS2_LAG[1], rs_stage2)
        stage(s, base, finish_out)
        stage(s, base + AG2_LAG[0], ag_stage1)
        stage(s, base + AG2_LAG[1], ag_stage2)
        stage(s, base + AG2_LAG[2], store_out)
        return carry

    lax.fori_loop(0, n_chunk + base + AG2_LAG[2], down_body, 0)


RS1_LAG = (2, 6, 10)
AG1_LAG = (2, 4, 5)
RS2_LAG = (2, 5, 8)
AG2_LAG = (2, 4, 5)
OUT_AHEAD = 4
LOAD_LAG = 4


def layer_tail(attn_out, resid_in, gain_mlp, w_out, w_gate, w_up, w_down):
    n_rows, width = resid_in.shape
    ffn = w_gate.shape[1]
    chunk = width // N_CHUNK
    half = chunk // 2
    rows = n_rows // 8
    f32, bf16 = jnp.float32, jnp.bfloat16
    vmem = pl.BlockSpec(memory_space=pltpu.VMEM)
    hbm = pl.BlockSpec(memory_space=pl.ANY)
    dma = pltpu.SemaphoreType.DMA
    return pl.pallas_call(
        tail_kernel,
        out_shape=jax.ShapeDtypeStruct((n_rows, width), bf16),
        in_specs=[vmem, hbm, vmem, hbm, hbm, hbm, hbm],
        out_specs=vmem,
        scratch_shapes=[
            pltpu.VMEM((N_CHUNK, 2, 2, 2, rows, chunk), f32),
            pltpu.VMEM((N_CHUNK, 2, 2, rows, chunk), f32),
            pltpu.VMEM((N_CHUNK, 2, 2, rows, half), f32),
            pltpu.VMEM((N_CHUNK, 2, rows, half), f32),
            pltpu.VMEM((N_CHUNK, 2, 2, 2, rows, chunk), f32),
            pltpu.VMEM((N_CHUNK, rows, chunk), f32),
            pltpu.VMEM((rows, chunk), f32),
            pltpu.VMEM((rows, width), bf16),
            pltpu.VMEM((width // 128, 128), f32),
            pltpu.VMEM((T_ROWS, n_rows), f32),
            pltpu.VMEM((T_ROWS, n_rows), f32),
            pltpu.VMEM((n_rows, ffn - T_ROWS), f32),
            pltpu.VMEM((n_rows, ffn - T_ROWS), f32),
            pltpu.VMEM((2, chunk, ffn - T_ROWS), bf16),
            pltpu.VMEM((n_rows, ffn), bf16),
            pltpu.VMEM((N_SLOT, ffn, chunk), bf16),
            dma(()),
            dma((N_CHUNK,)),
            dma((N_SLOT,)),
            dma((N_CHUNK,)),
            dma((3, N_CHUNK)),
            dma((N_CHUNK,)),
            dma((3, N_CHUNK)),
        ],
        compiler_params=pltpu.CompilerParams(collective_id=0, has_side_effects=True,
                                             vmem_limit_bytes=53477376),
        name='layer_tail',
    )(attn_out, resid_in, gain_mlp.reshape(width // 128, 128), w_out, w_gate.T, w_up.T, w_down)


def solution(mesh):
    def layer_local(resid_in, positions, k_cache, v_cache, gain_attn, w_query, w_key, w_value,
                    w_out, gain_mlp, w_gate, w_up, w_down):
        attn_out, k_full, v_full = layer_front(resid_in, positions, k_cache, v_cache,
                                               gain_attn, w_query, w_key, w_value)
        resid_out = layer_tail(attn_out, resid_in, gain_mlp, w_out, w_gate, w_up, w_down)
        return resid_out, k_full, v_full

    row_spec = P('dp', None)
    cache_spec = P('dp', None, 'tp', None)
    col_spec = P(None, 'tp')
    split_rows = P('tp', None)
    return jax.shard_map(layer_local, mesh=mesh,
                         in_specs=(row_spec, P('dp'), cache_spec, cache_spec, P(), col_spec, col_spec,
                                   col_spec, split_rows, P(), col_spec, col_spec, split_rows),
                         out_specs=(row_spec, cache_spec, cache_spec), check_vma=False)
```

```python
import math
import jax
import jax.numpy as jnp
from jax import lax
from jax.experimental import pallas as pl
from jax.experimental.pallas import tpu as pltpu
from jax.sharding import PartitionSpec as P

EPS = 1e-5
ROPE_THETA = 500000.0
ROPE_FACTOR = 8.0
LOW_FACTOR = 1.0
HIGH_FACTOR = 4.0
ORIG_CTX = 8192.0


def rope_freqs(head_dim):
    half_dim = head_dim // 2
    exponents = (jnp.arange(head_dim, dtype=jnp.int32) % half_dim).astype(jnp.float32) * (2.0 / head_dim)
    inv_freq = 1.0 / jnp.power(ROPE_THETA, exponents)
    wavelen = (2.0 * math.pi) / inv_freq
    smooth = (ORIG_CTX / wavelen - LOW_FACTOR) / (HIGH_FACTOR - LOW_FACTOR)
    blended = (1.0 - smooth) * inv_freq / ROPE_FACTOR + smooth * inv_freq
    inv_freq = jnp.where(wavelen < ORIG_CTX / HIGH_FACTOR, inv_freq,
                         jnp.where(wavelen > ORIG_CTX / LOW_FACTOR, inv_freq / ROPE_FACTOR, blended))
    return inv_freq[None, :]


def front_kernel(pos_ref, resid_hbm, gain_hbm, pos_row_hbm, freq_ref, w_query_hbm, w_key_hbm, w_value_hbm,
                 k_in_hbm, v_in_hbm, attn_ref, k_out_hbm, v_out_hbm,
                 w_buf, acc, k_buf, v_buf, q_rows, o_rows, k_new, v_new, gain_f, cos_ref, sin_ref, resid_ref, gain_ref, pos_row_ref,
                 small_sem, resid_sem, w_sem, cache_sem, out_sem):
    n_seqs, width = resid_ref.shape
    depth, q_width = w_buf.shape[1], w_query_hbm.shape[1]
    head_dim = k_new.shape[1]
    group_size = q_width // head_dim
    n_block = n_seqs // SEQ_BLOCK

    def w_copies(c):
        span = pl.ds(pl.multiple_of(c * depth, depth), depth)
        copies = []
        for i, (src, lo, size) in enumerate(((w_query_hbm, 0, q_width), (w_key_hbm, q_width, head_dim),
                                             (w_value_hbm, q_width + head_dim, head_dim))):
            copies.append(pltpu.make_async_copy(src.at[span], w_buf.at[c, :, pl.ds(lo, size)], w_sem.at[i, c]))
        return copies

    def block(b):
        return pl.ds(pl.multiple_of(b * SEQ_BLOCK, SEQ_BLOCK), SEQ_BLOCK)

    def in_copies(b):
        return (pltpu.make_async_copy(k_in_hbm.at[block(b)], k_buf.at[block(b)], cache_sem.at[0, b]),
                pltpu.make_async_copy(v_in_hbm.at[block(b)], v_buf.at[block(b)], cache_sem.at[1, b]))

    def out_copies(b):
        return (pltpu.make_async_copy(k_buf.at[block(b)], k_out_hbm.at[block(b)], out_sem.at[0, b]),
                pltpu.make_async_copy(v_buf.at[block(b)], v_out_hbm.at[block(b)], out_sem.at[1, b]))

    n_w = width // depth
    def cols(c):
        return pl.ds(pl.multiple_of(c * depth, depth), depth)

    def resid_copy(c):
        return pltpu.make_async_copy(resid_hbm.at[:, cols(c)], resid_ref.at[:, cols(c)], resid_sem.at[c])

    small_copies = [pltpu.make_async_copy(pos_row_hbm, pos_row_ref, small_sem.at[0]),
                    pltpu.make_async_copy(gain_hbm, gain_ref, small_sem.at[1])]
    for copy in small_copies:
        copy.start()
    for c in range(n_w):
        resid_copy(c).start()
    for c in range(2):
        for copy in w_copies(c):
            copy.start()
    for copy in small_copies:
        copy.wait()
    gain_f[...] = gain_ref[...].astype(jnp.float32)

    def add_squares(c, total):
        resid_copy(c).wait()
        part = resid_ref[:, cols(c)].astype(jnp.float32)
        part = part * part
        for j in range(depth // 128):
            total = total + part[:, j * 128:(j + 1) * 128]
        return total

    acc[...] = jnp.zeros_like(acc)
    angles = (jnp.broadcast_to(pos_row_ref[...].astype(jnp.float32), (n_seqs, n_seqs)).T[:, :1]
              * freq_ref[...])
    cos_f = jnp.cos(angles)
    sin_f = jnp.sin(angles)
    sin_f = jnp.where(lax.broadcasted_iota(jnp.int32, sin_f.shape, 1) < head_dim // 2, -sin_f, sin_f)
    cos_ref[...] = cos_f
    sin_ref[...] = sin_f
    squares = lax.fori_loop(0, n_w, add_squares, jnp.zeros((n_seqs, 128), jnp.float32))
    for c in range(2, W_AHEAD):
        for copy in w_copies(c):
            copy.start()
    scale = lax.rsqrt(jnp.sum(squares, axis=-1, keepdims=True) * (1.0 / width) + EPS)
    per_step = n_block // (n_w // 2)

    def project(c, carry):
        rows_f = resid_ref[:, cols(c)].astype(jnp.float32) * scale
        normed = jnp.concatenate(
            [rows_f[:, j * 128:(j + 1) * 128] * gain_f[pl.ds(c * (depth // 128) + j, 1), :]
             for j in range(depth // 128)], axis=-1).astype(jnp.bfloat16)
        for copy in w_copies(c):
            copy.wait()

        @pl.when(c + W_AHEAD < n_w)
        def _():
            for copy in w_copies(c + W_AHEAD):
                copy.start()

        @pl.when(c >= n_w // 2)
        def _():
            for i in range(per_step):
                for copy in in_copies((c - n_w // 2) * per_step + i):
                    copy.start()

        acc[...] += jnp.dot(normed, w_buf[c], preferred_element_type=jnp.float32)
        return carry

    lax.fori_loop(0, n_w, project, 0)

    def rotate(cols_f):
        values = cols_f.astype(jnp.bfloat16).astype(jnp.float32)
        turned = values * cos_ref[...] + pltpu.roll(values, head_dim // 2, 1) * sin_ref[...]
        return turned.astype(jnp.bfloat16).astype(jnp.float32)

    for j in range(group_size):
        q_rows[pl.ds(j, n_seqs, stride=group_size), :] = rotate(acc[:, j * head_dim:(j + 1) * head_dim])
    k_new[...] = rotate(acc[:, q_width:q_width + head_dim])
    v_new[...] = acc[:, q_width + head_dim:].astype(jnp.bfloat16).astype(jnp.float32)
    inv_sqrt = 1.0 / math.sqrt(head_dim)

    def attend(b, carry):
        for copy in in_copies(b):
            copy.wait()
        for i in range(SEQ_BLOCK):
            seq = b * SEQ_BLOCK + i
            pos = pos_ref[seq]
            base = pl.multiple_of(pos // 16 * 16, 16)
            hit = lax.broadcasted_iota(jnp.int32, (16, head_dim), 0) == pos - base
            for buf, new in ((k_buf, k_new), (v_buf, v_new)):
                old = buf[seq, pl.ds(base, 16), :].astype(jnp.float32)
                buf[seq, pl.ds(base, 16), :] = jnp.where(hit, new[pl.ds(seq, 1), :], old).astype(jnp.bfloat16)
        for copy in out_copies(b):
            copy.start()
        rows, probs = [], []
        for i in range(SEQ_BLOCK):
            seq = b * SEQ_BLOCK + i
            rows.append(pl.ds(pl.multiple_of(seq * group_size, group_size), group_size))
            query = q_rows[rows[i], :].astype(jnp.bfloat16)
            scores = lax.dot_general(query, k_buf[seq], (((1,), (1,)), ((), ())),
                                     preferred_element_type=jnp.float32) * inv_sqrt
            valid = lax.broadcasted_iota(jnp.int32, scores.shape, 1) <= pos_ref[seq]
            scores = jnp.where(valid, scores, -jnp.inf)
            exps = jnp.exp(scores - jnp.max(scores, axis=-1, keepdims=True))
            probs.append((exps / jnp.sum(exps, axis=-1, keepdims=True)).astype(jnp.bfloat16))
        for i in range(SEQ_BLOCK):
            o_rows[rows[i], :] = jnp.dot(probs[i], v_buf[b * SEQ_BLOCK + i], preferred_element_type=jnp.float32)
        return carry

    lax.fori_loop(0, n_block, attend, 0)
    for j in range(group_size):
        attn_ref[:, j * head_dim:(j + 1) * head_dim] = (
            o_rows[pl.ds(j, n_seqs, stride=group_size), :].astype(jnp.bfloat16))
    for b in range(n_block):
        for copy in out_copies(b):
            copy.wait()


SEQ_BLOCK = 32
FRONT_DEPTH = 1024
W_AHEAD = 4


def layer_front(resid_in, positions, k_cache, v_cache, gain_attn, w_query, w_key, w_value):
    n_seqs, width = resid_in.shape
    cache_len, head_dim = k_cache.shape[1], k_cache.shape[3]
    q_width = w_query.shape[1]
    f32, bf16 = jnp.float32, jnp.bfloat16
    vmem = pl.BlockSpec(memory_space=pltpu.VMEM)
    hbm = pl.BlockSpec(memory_space=pl.ANY)
    dma = pltpu.SemaphoreType.DMA
    n_w, n_block = width // FRONT_DEPTH, n_seqs // SEQ_BLOCK
    flat = (n_seqs, cache_len, head_dim)
    attn_out, k_out, v_out = pl.pallas_call(
        front_kernel,
        out_shape=(jax.ShapeDtypeStruct((n_seqs, q_width), bf16),
                   jax.ShapeDtypeStruct(flat, bf16), jax.ShapeDtypeStruct(flat, bf16)),
        in_specs=[pl.BlockSpec(memory_space=pltpu.SMEM), hbm, hbm, hbm, vmem, hbm, hbm, hbm, hbm, hbm],
        out_specs=(vmem, hbm, hbm),
        scratch_shapes=[
            pltpu.VMEM((n_w, FRONT_DEPTH, q_width + 2 * head_dim), bf16),
            pltpu.VMEM((n_seqs, q_width + 2 * head_dim), f32),
            pltpu.VMEM(flat, bf16),
            pltpu.VMEM(flat, bf16),
            pltpu.VMEM((n_seqs * q_width // head_dim, head_dim), f32),
            pltpu.VMEM((n_seqs * q_width // head_dim, head_dim), f32),
            pltpu.VMEM((n_seqs, head_dim), f32),
            pltpu.VMEM((n_seqs, head_dim), f32),
            pltpu.VMEM((width // 128, 128), f32),
            pltpu.VMEM((n_seqs, head_dim), f32),
            pltpu.VMEM((n_seqs, head_dim), f32),
            pltpu.VMEM((n_seqs, width), bf16),
            pltpu.VMEM((width // 128, 128), bf16),
            pltpu.VMEM((1, n_seqs), jnp.int32),
            dma((2,)),
            dma((n_w,)),
            dma((3, n_w)),
            dma((2, n_block)),
            dma((2, n_block)),
        ],
        compiler_params=pltpu.CompilerParams(vmem_limit_bytes=55050240),
        name='layer_front',
    )(positions, resid_in, pltpu.with_memory_space_constraint(gain_attn.reshape(width // 128, 128), pltpu.HBM),
      pltpu.with_memory_space_constraint(positions[None, :], pltpu.HBM),
      rope_freqs(head_dim), w_query, w_key, w_value,
      k_cache.reshape(flat), v_cache.reshape(flat))
    return attn_out, k_out.reshape(k_cache.shape), v_out.reshape(v_cache.shape)


N_CHUNK = 16
N_SLOT = 11
T_ROWS = 1024
MESH = pl.DeviceIdType.MESH


def tail_kernel(attn_ref, resid_hbm, gain_ref, w_out_hbm, gate_t_hbm, up_t_hbm, w_down_hbm, out_ref,
                part, from_core, from_1, from_2, gathered, mid, sq_sum, resid_own, gain_f,
                gate_acc, up_acc, gate_acc_t, up_acc_t, turned, hidden, ring,
                resid_sem, out_sem, ring_sem, rs_send, rs_recv, ag_send, ag_recv):
    n_chunk, chunk = N_CHUNK, part.shape[-1]
    half = chunk // 2
    rows = mid.shape[1]
    me = lax.axis_index('tp')
    k = me % 2
    x = (me // 2) % 2
    y = me // 4
    nk, nx, ny = 1 - k, 1 - x, 1 - y
    core_nbr = {'tp': me + 1 - 2 * k}
    x_nbr = {'tp': me + 2 - 4 * x}
    y_nbr = {'tp': me + 4 - 8 * y}
    far_nbr = {'tp': me + 6 - 4 * x - 8 * y}

    def cols(c):
        return pl.ds(pl.multiple_of(c * chunk, chunk), chunk)

    depth_out = w_out_hbm.shape[0]
    first_mlp = n_chunk // 2
    first_down = first_mlp + 2 * n_chunk

    def out_slot(c):
        return c // 2, pl.ds(pl.multiple_of((c % 2) * depth_out, depth_out), depth_out)

    def out_copy(c):
        slot, span = out_slot(c)
        return pltpu.make_async_copy(w_out_hbm.at[:, cols(c)], ring.at[slot, span], out_sem.at[c % OUT_AHEAD])

    def ring_copy(src, c, j):
        slot = j % N_SLOT
        return pltpu.make_async_copy(src.at[:, cols(c)], ring.at[slot], ring_sem.at[slot])

    def gate_copy(c):
        return ring_copy(gate_t_hbm, c, first_mlp + 2 * c)

    def up_copy(c):
        return ring_copy(up_t_hbm, c, first_mlp + 2 * c + 1)

    def down_copy(c):
        return ring_copy(w_down_hbm, c, first_down + c)

    def start_load(j):
        m = j - first_mlp

        @pl.when(j < first_down)
        def _():
            @pl.when(m % 2 == 0)
            def _():
                gate_copy(m // 2).start()

            @pl.when(m % 2 == 1)
            def _():
                up_copy(m // 2).start()

        @pl.when(jnp.logical_and(j >= first_down, j < first_down + n_chunk))
        def _():
            down_copy(j - first_down).start()

    row0 = pl.multiple_of(64 * k + 32 * x + 16 * y, 16)
    resid_copy = pltpu.make_async_copy(resid_hbm.at[pl.ds(row0, rows)], resid_own, resid_sem)
    out_copy(0).start()

    barrier = pltpu.get_barrier_semaphore()
    for nbr in (core_nbr, x_nbr, y_nbr, far_nbr):
        pl.semaphore_signal(barrier, inc=1, device_id=nbr, device_id_type=MESH)

    def remote(src, dst, sems, ch, c, nbr):
        return pltpu.make_async_remote_copy(src_ref=src, dst_ref=dst, send_sem=sems[0].at[c],
                                            recv_sem=sems[1].at[ch, c], device_id=nbr, device_id_type=MESH)

    def wait_bytes(ref, sem):
        pltpu.make_async_copy(ref, ref, sem).wait()

    def wait_sent(sems, c):
        wait_bytes(mid.at[pl.ds(0, 7)], sems[0].at[c])

    rs = (rs_send, rs_recv)
    ag = (ag_send, ag_recv)
    left, right = pl.ds(0, half), pl.ds(half, half)

    def rs_core(c):
        return remote(part.at[c, nk], from_core.at[c], rs, 0, c, core_nbr)

    def rs_x1(c):
        return remote(part.at[c, k, nx, :, :, left], from_1.at[c, 0], rs, 1, c, x_nbr)

    def rs_y1(c):
        return remote(part.at[c, k, :, ny, :, right], from_1.at[c, 1], rs, 1, c, y_nbr)

    def rs_y2(c):
        return remote(part.at[c, k, x, ny, :, left], from_2.at[c, 0], rs, 2, c, y_nbr)

    def rs_x2(c):
        return remote(part.at[c, k, nx, y, :, right], from_2.at[c, 1], rs, 2, c, x_nbr)

    def ag_x(c):
        blk = gathered.at[c, k, x, y]
        return remote(blk, blk, ag, 0, c, x_nbr)

    def ag_y(c):
        blk = gathered.at[c, k, x, y]
        return remote(blk, blk, ag, 0, c, y_nbr)

    def ag_far(c):
        blk = gathered.at[c, k, x, y]
        return remote(blk, blk, ag, 1, c, far_nbr)

    def ag_fwd_y(c):
        blk = gathered.at[c, k, nx, y, :, right]
        return remote(blk, blk, ag, 1, c, y_nbr)

    def ag_fwd_x(c):
        blk = gathered.at[c, k, x, ny, :, left]
        return remote(blk, blk, ag, 1, c, x_nbr)

    def ag_core(c):
        blk = gathered.at[c, k]
        return remote(blk, blk, ag, 2, c, core_nbr)

    def stage(s, lag, fn):
        c = s - lag

        @pl.when(jnp.logical_and(c >= 0, c < n_chunk))
        def _():
            fn(c)

    def rs_stage1(c):
        rs_core(c).wait_recv()
        part[c, k] = part[c, k] + from_core[c]
        rs_x1(c).start()
        rs_y1(c).start()

    def rs_stage2(c):
        wait_bytes(from_1.at[c], rs_recv.at[1, c])
        part[c, k, x, :, :, left] = part[c, k, x, :, :, left] + from_1[c, 0]
        part[c, k, :, y, :, right] = part[c, k, :, y, :, right] + from_1[c, 1]
        rs_y2(c).start()
        rs_x2(c).start()

    def rs_stage3(c):
        wait_bytes(from_2.at[c], rs_recv.at[2, c])
        total = jnp.concatenate([part[c, k, x, y, :, left] + from_2[c, 0],
                                 part[c, k, x, y, :, right] + from_2[c, 1]], axis=-1)
        wait_sent(rs, c)
        return total

    def ag_stage1(c):
        wait_bytes(from_1.at[c], ag_recv.at[0, c])
        ag_fwd_y(c).start()
        ag_fwd_x(c).start()

    def ag_stage2(c):
        wait_bytes(from_2.at[c], ag_recv.at[1, c])
        ag_core(c).start()

    def ag_stage3(c):
        ag_core(c).wait_recv()
        block = gathered[c].reshape(8 * rows, chunk)
        wait_sent(ag, c)
        return block

    gain_f[...] = gain_ref[...].astype(jnp.float32)
    sq_sum[...] = jnp.zeros_like(sq_sum)
    gate_acc[...] = jnp.zeros_like(gate_acc)
    up_acc[...] = jnp.zeros_like(up_acc)
    gate_acc_t[...] = jnp.zeros_like(gate_acc_t)
    up_acc_t[...] = jnp.zeros_like(up_acc_t)
    for c in range(1, OUT_AHEAD):
        out_copy(c).start()
    resid_copy.start()
    pl.semaphore_wait(barrier, 4)

    def proj(c):
        out_copy(c).wait()
        slot, span = out_slot(c)
        res = jnp.dot(attn_ref[...], ring[slot, span], preferred_element_type=jnp.float32)
        part[c] = res.reshape(part.shape[1:])
        rs_core(c).start()

        @pl.when(c + OUT_AHEAD < n_chunk)
        def _():
            out_copy(c + OUT_AHEAD).start()

        ahead = first_mlp + c - LOAD_LAG

        @pl.when(jnp.logical_and(c >= LOAD_LAG, ahead < N_SLOT))
        def _():
            start_load(ahead)

        @pl.when(c % 2 == 1)
        def _():
            start_load(c // 2 + N_SLOT)

    def finish_mid(c):
        @pl.when(c == 0)
        def _():
            resid_copy.wait()

        total = rs_stage3(c)
        x1 = (resid_own[:, cols(c)].astype(jnp.float32) + total).astype(jnp.bfloat16).astype(jnp.float32)
        mid[c] = x1
        sq_sum[...] += x1 * x1

    def rs_body(s, carry):
        stage(s, 0, proj)
        stage(s, RS1_LAG[0], rs_stage1)
        stage(s, RS1_LAG[1], rs_stage2)
        stage(s, RS1_LAG[2], finish_mid)
        return carry

    lax.fori_loop(0, n_chunk + RS1_LAG[2], rs_body, 0)

    mean_sq = jnp.sum(sq_sum[...], axis=-1, keepdims=True) * (1.0 / (n_chunk * chunk))
    scale = lax.rsqrt(mean_sq + EPS)

    def send_normed(c):
        gain = jnp.concatenate([gain_f[pl.ds(c * (chunk // 128) + j, 1), :] for j in range(chunk // 128)], axis=-1)
        normed = (mid[c] * scale * gain).astype(jnp.bfloat16)
        gathered[c, k, x, y] = normed.astype(jnp.float32)
        ag_x(c).start()
        ag_y(c).start()

    def gate_up(c):
        block = ag_stage3(c).astype(jnp.bfloat16)
        gate_copy(c).wait()
        up_copy(c).wait()
        first = first_mlp + 2 * c
        accs = ((gate_acc, gate_acc_t), (up_acc, up_acc_t))
        for i, (acc, acc_t) in enumerate(accs):
            slot = (first + i) % N_SLOT
            turned[i] = ring[slot, pl.ds(T_ROWS, acc_t.shape[1])].T
            acc[...] += lax.dot_general(ring[slot, pl.ds(0, T_ROWS)], block, (((1,), (1,)), ((), ())),
                                        preferred_element_type=jnp.float32)
        for i, (acc, acc_t) in enumerate(accs):
            acc_t[...] += jnp.dot(block, turned[i], preferred_element_type=jnp.float32)
        for i in range(2):
            start_load(first + i + N_SLOT)

    def ag_body(s, carry):
        stage(s, 0, send_normed)
        stage(s, AG1_LAG[0], ag_stage1)
        stage(s, AG1_LAG[1], ag_stage2)
        stage(s, AG1_LAG[2], gate_up)
        return carry

    lax.fori_loop(0, n_chunk + AG1_LAG[2], ag_body, 0)

    def act(gate, up):
        gate = gate.astype(jnp.bfloat16).astype(jnp.float32)
        up = up.astype(jnp.bfloat16).astype(jnp.float32)
        return jax.nn.silu(gate) * up

    for lo in range(0, T_ROWS, 128):
        span = slice(lo, lo + 128)
        hidden[:, span] = act(gate_acc[span, :], up_acc[span, :]).T.astype(jnp.bfloat16)
    hidden[:, T_ROWS:] = act(gate_acc_t[...], up_acc_t[...]).astype(jnp.bfloat16)

    def down(c):
        down_copy(c).wait()
        j = first_down + c
        res = jnp.dot(hidden[...], ring[j % N_SLOT], preferred_element_type=jnp.float32)
        part[c] = res.reshape(part.shape[1:])
        rs_core(c).start()
        start_load(j + N_SLOT)

    def finish_out(c):
        total = rs_stage3(c)
        gathered[c, k, x, y] = (mid[c] + total).astype(jnp.bfloat16).astype(jnp.float32)
        ag_x(c).start()
        ag_y(c).start()

        @pl.when(c == n_chunk - 1)
        def _():
            ag_far(c).start()

    def ag_stage1_out(c):
        wait_bytes(from_1.at[c], ag_recv.at[0, c])

        @pl.when(c < n_chunk - 1)
        def _():
            ag_fwd_y(c).start()
            ag_fwd_x(c).start()

    def store_out(c):
        out_ref[:, cols(c)] = ag_stage3(c).astype(jnp.bfloat16)

    base = RS2_LAG[2]

    def down_body(s, carry):
        stage(s, 0, down)
        stage(s, RS2_LAG[0], rs_stage1)
        stage(s, RS2_LAG[1], rs_stage2)
        stage(s, base, finish_out)
        stage(s, base + AG2_LAG[0], ag_stage1_out)
        stage(s, base + AG2_LAG[1], ag_stage2)
        stage(s, base + AG2_LAG[2], store_out)
        return carry

    lax.fori_loop(0, n_chunk + base + AG2_LAG[2], down_body, 0)


RS1_LAG = (2, 6, 10)
AG1_LAG = (2, 4, 5)
RS2_LAG = (2, 5, 8)
AG2_LAG = (2, 4, 5)
OUT_AHEAD = 4
LOAD_LAG = 4


def layer_tail(attn_out, resid_in, gain_mlp, w_out, w_gate, w_up, w_down):
    n_rows, width = resid_in.shape
    ffn = w_gate.shape[1]
    chunk = width // N_CHUNK
    half = chunk // 2
    rows = n_rows // 8
    f32, bf16 = jnp.float32, jnp.bfloat16
    vmem = pl.BlockSpec(memory_space=pltpu.VMEM)
    hbm = pl.BlockSpec(memory_space=pl.ANY)
    dma = pltpu.SemaphoreType.DMA
    return pl.pallas_call(
        tail_kernel,
        out_shape=jax.ShapeDtypeStruct((n_rows, width), bf16),
        in_specs=[vmem, hbm, vmem, hbm, hbm, hbm, hbm],
        out_specs=vmem,
        scratch_shapes=[
            pltpu.VMEM((N_CHUNK, 2, 2, 2, rows, chunk), f32),
            pltpu.VMEM((N_CHUNK, 2, 2, rows, chunk), f32),
            pltpu.VMEM((N_CHUNK, 2, 2, rows, half), f32),
            pltpu.VMEM((N_CHUNK, 2, rows, half), f32),
            pltpu.VMEM((N_CHUNK, 2, 2, 2, rows, chunk), f32),
            pltpu.VMEM((N_CHUNK, rows, chunk), f32),
            pltpu.VMEM((rows, chunk), f32),
            pltpu.VMEM((rows, width), bf16),
            pltpu.VMEM((width // 128, 128), f32),
            pltpu.VMEM((T_ROWS, n_rows), f32),
            pltpu.VMEM((T_ROWS, n_rows), f32),
            pltpu.VMEM((n_rows, ffn - T_ROWS), f32),
            pltpu.VMEM((n_rows, ffn - T_ROWS), f32),
            pltpu.VMEM((2, chunk, ffn - T_ROWS), bf16),
            pltpu.VMEM((n_rows, ffn), bf16),
            pltpu.VMEM((N_SLOT, ffn, chunk), bf16),
            dma(()),
            dma((OUT_AHEAD,)),
            dma((N_SLOT,)),
            dma((N_CHUNK,)),
            dma((3, N_CHUNK)),
            dma((N_CHUNK,)),
            dma((3, N_CHUNK)),
        ],
        compiler_params=pltpu.CompilerParams(collective_id=0, has_side_effects=True,
                                             vmem_limit_bytes=53477376),
        name='layer_tail',
    )(attn_out, resid_in, gain_mlp.reshape(width // 128, 128), w_out, w_gate.T, w_up.T, w_down)


def solution(mesh):
    def layer_local(resid_in, positions, k_cache, v_cache, gain_attn, w_query, w_key, w_value,
                    w_out, gain_mlp, w_gate, w_up, w_down):
        attn_out, k_full, v_full = layer_front(resid_in, positions, k_cache, v_cache,
                                               gain_attn, w_query, w_key, w_value)
        resid_out = layer_tail(attn_out, resid_in, gain_mlp, w_out, w_gate, w_up, w_down)
        return resid_out, k_full, v_full

    row_spec = P('dp', None)
    cache_spec = P('dp', None, 'tp', None)
    col_spec = P(None, 'tp')
    split_rows = P('tp', None)
    return jax.shard_map(layer_local, mesh=mesh,
                         in_specs=(row_spec, P('dp'), cache_spec, cache_spec, P(), col_spec, col_spec,
                                   col_spec, split_rows, P(), col_spec, col_spec, split_rows),
                         out_specs=(row_spec, cache_spec, cache_spec), check_vma=False)
```

```python
import math
import jax
import jax.numpy as jnp
from jax import lax
from jax.experimental import pallas as pl
from jax.experimental.pallas import tpu as pltpu
from jax.sharding import PartitionSpec as P

EPS = 1e-5
ROPE_THETA = 500000.0
ROPE_FACTOR = 8.0
LOW_FACTOR = 1.0
HIGH_FACTOR = 4.0
ORIG_CTX = 8192.0


def rope_freqs(head_dim):
    half_dim = head_dim // 2
    exponents = (jnp.arange(head_dim, dtype=jnp.int32) % half_dim).astype(jnp.float32) * (2.0 / head_dim)
    inv_freq = 1.0 / jnp.power(ROPE_THETA, exponents)
    wavelen = (2.0 * math.pi) / inv_freq
    smooth = (ORIG_CTX / wavelen - LOW_FACTOR) / (HIGH_FACTOR - LOW_FACTOR)
    blended = (1.0 - smooth) * inv_freq / ROPE_FACTOR + smooth * inv_freq
    inv_freq = jnp.where(wavelen < ORIG_CTX / HIGH_FACTOR, inv_freq,
                         jnp.where(wavelen > ORIG_CTX / LOW_FACTOR, inv_freq / ROPE_FACTOR, blended))
    return inv_freq[None, :]


def front_kernel(pos_ref, resid_hbm, gain_ref, pos_row_ref, freq_ref, w_query_hbm, w_key_hbm, w_value_hbm,
                 k_in_hbm, v_in_hbm, attn_ref, k_out_hbm, v_out_hbm,
                 w_buf, acc, k_buf, v_buf, q_rows, o_rows, k_new, v_new, gain_f, cos_ref, sin_ref, resid_ref,
                 resid_sem, w_sem, cache_sem, out_sem):
    n_seqs, width = resid_ref.shape
    depth, q_width = w_buf.shape[1], w_query_hbm.shape[1]
    head_dim = k_new.shape[1]
    group_size = q_width // head_dim
    n_block = n_seqs // SEQ_BLOCK

    def w_copies(c):
        span = pl.ds(pl.multiple_of(c * depth, depth), depth)
        copies = []
        for i, (src, lo, size) in enumerate(((w_query_hbm, 0, q_width), (w_key_hbm, q_width, head_dim),
                                             (w_value_hbm, q_width + head_dim, head_dim))):
            copies.append(pltpu.make_async_copy(src.at[span], w_buf.at[c, :, pl.ds(lo, size)], w_sem.at[i, c]))
        return copies

    def block(b):
        return pl.ds(pl.multiple_of(b * SEQ_BLOCK, SEQ_BLOCK), SEQ_BLOCK)

    def in_copies(b):
        return (pltpu.make_async_copy(k_in_hbm.at[block(b)], k_buf.at[block(b)], cache_sem.at[0, b]),
                pltpu.make_async_copy(v_in_hbm.at[block(b)], v_buf.at[block(b)], cache_sem.at[1, b]))

    def out_copies(b):
        return (pltpu.make_async_copy(k_buf.at[block(b)], k_out_hbm.at[block(b)], out_sem.at[0, b]),
                pltpu.make_async_copy(v_buf.at[block(b)], v_out_hbm.at[block(b)], out_sem.at[1, b]))

    n_w = width // depth

    def resid_copy(c):
        span = pl.ds(pl.multiple_of(c * depth, depth), depth)
        return pltpu.make_async_copy(resid_hbm.at[:, span], resid_ref.at[:, span], resid_sem.at[c])

    for c in range(n_w):
        resid_copy(c).start()
    for copy in w_copies(0):
        copy.start()
    gain_f[...] = gain_ref[...].astype(jnp.float32)

    def cols(c):
        return pl.ds(pl.multiple_of(c * depth, depth), depth)

    def add_squares(c, total):
        resid_copy(c).wait()
        part = resid_ref[:, cols(c)].astype(jnp.float32)
        part = part * part
        for j in range(depth // 128):
            total = total + part[:, j * 128:(j + 1) * 128]
        return total

    acc[...] = jnp.zeros_like(acc)
    angles = (jnp.broadcast_to(pos_row_ref[...].astype(jnp.float32), (n_seqs, n_seqs)).T[:, :1]
              * freq_ref[...])
    cos_f = jnp.cos(angles)
    sin_f = jnp.sin(angles)
    sin_f = jnp.where(lax.broadcasted_iota(jnp.int32, sin_f.shape, 1) < head_dim // 2, -sin_f, sin_f)
    cos_ref[...] = cos_f
    sin_ref[...] = sin_f
    for c in range(1, W_AHEAD):
        for copy in w_copies(c):
            copy.start()
    squares = lax.fori_loop(0, n_w, add_squares, jnp.zeros((n_seqs, 128), jnp.float32))
    scale = lax.rsqrt(jnp.sum(squares, axis=-1, keepdims=True) * (1.0 / width) + EPS)
    per_step = n_block // (n_w // 2)

    def project(c, carry):
        rows_f = resid_ref[:, cols(c)].astype(jnp.float32) * scale
        normed = jnp.concatenate(
            [rows_f[:, j * 128:(j + 1) * 128] * gain_f[pl.ds(c * (depth // 128) + j, 1), :]
             for j in range(depth // 128)], axis=-1).astype(jnp.bfloat16)
        for copy in w_copies(c):
            copy.wait()

        @pl.when(c + W_AHEAD < n_w)
        def _():
            for copy in w_copies(c + W_AHEAD):
                copy.start()

        @pl.when(c >= n_w // 2)
        def _():
            for i in range(per_step):
                for copy in in_copies((c - n_w // 2) * per_step + i):
                    copy.start()

        acc[...] += jnp.dot(normed, w_buf[c], preferred_element_type=jnp.float32)
        return carry

    lax.fori_loop(0, n_w, project, 0)

    def rotate(cols_f):
        values = cols_f.astype(jnp.bfloat16).astype(jnp.float32)
        turned = values * cos_ref[...] + pltpu.roll(values, head_dim // 2, 1) * sin_ref[...]
        return turned.astype(jnp.bfloat16).astype(jnp.float32)

    for j in range(group_size):
        q_rows[pl.ds(j, n_seqs, stride=group_size), :] = rotate(acc[:, j * head_dim:(j + 1) * head_dim])
    k_new[...] = rotate(acc[:, q_width:q_width + head_dim])
    v_new[...] = acc[:, q_width + head_dim:].astype(jnp.bfloat16).astype(jnp.float32)
    inv_sqrt = 1.0 / math.sqrt(head_dim)

    def attend(b, carry):
        for copy in in_copies(b):
            copy.wait()
        for i in range(SEQ_BLOCK):
            seq = b * SEQ_BLOCK + i
            pos = pos_ref[seq]
            base = pl.multiple_of(pos // 16 * 16, 16)
            hit = lax.broadcasted_iota(jnp.int32, (16, head_dim), 0) == pos - base
            for buf, new in ((k_buf, k_new), (v_buf, v_new)):
                old = buf[seq, pl.ds(base, 16), :].astype(jnp.float32)
                buf[seq, pl.ds(base, 16), :] = jnp.where(hit, new[pl.ds(seq, 1), :], old).astype(jnp.bfloat16)
        for copy in out_copies(b):
            copy.start()
        rows, probs = [], []
        for i in range(SEQ_BLOCK):
            seq = b * SEQ_BLOCK + i
            rows.append(pl.ds(pl.multiple_of(seq * group_size, group_size), group_size))
            query = q_rows[rows[i], :].astype(jnp.bfloat16)
            scores = lax.dot_general(query, k_buf[seq], (((1,), (1,)), ((), ())),
                                     preferred_element_type=jnp.float32) * inv_sqrt
            valid = lax.broadcasted_iota(jnp.int32, scores.shape, 1) <= pos_ref[seq]
            scores = jnp.where(valid, scores, -jnp.inf)
            exps = jnp.exp(scores - jnp.max(scores, axis=-1, keepdims=True))
            probs.append((exps / jnp.sum(exps, axis=-1, keepdims=True)).astype(jnp.bfloat16))
        for i in range(SEQ_BLOCK):
            o_rows[rows[i], :] = jnp.dot(probs[i], v_buf[b * SEQ_BLOCK + i], preferred_element_type=jnp.float32)
        return carry

    lax.fori_loop(0, n_block, attend, 0)
    for j in range(group_size):
        attn_ref[:, j * head_dim:(j + 1) * head_dim] = (
            o_rows[pl.ds(j, n_seqs, stride=group_size), :].astype(jnp.bfloat16))
    for b in range(n_block):
        for copy in out_copies(b):
            copy.wait()


SEQ_BLOCK = 32
FRONT_DEPTH = 2048
W_AHEAD = 2


def layer_front(resid_in, positions, k_cache, v_cache, gain_attn, w_query, w_key, w_value):
    n_seqs, width = resid_in.shape
    cache_len, head_dim = k_cache.shape[1], k_cache.shape[3]
    q_width = w_query.shape[1]
    f32, bf16 = jnp.float32, jnp.bfloat16
    vmem = pl.BlockSpec(memory_space=pltpu.VMEM)
    hbm = pl.BlockSpec(memory_space=pl.ANY)
    dma = pltpu.SemaphoreType.DMA
    n_w, n_block = width // FRONT_DEPTH, n_seqs // SEQ_BLOCK
    flat = (n_seqs, cache_len, head_dim)
    attn_out, k_out, v_out = pl.pallas_call(
        front_kernel,
        out_shape=(jax.ShapeDtypeStruct((n_seqs, q_width), bf16),
                   jax.ShapeDtypeStruct(flat, bf16), jax.ShapeDtypeStruct(flat, bf16)),
        in_specs=[pl.BlockSpec(memory_space=pltpu.SMEM), hbm, vmem, vmem, vmem, hbm, hbm, hbm, hbm, hbm],
        out_specs=(vmem, hbm, hbm),
        scratch_shapes=[
            pltpu.VMEM((n_w, FRONT_DEPTH, q_width + 2 * head_dim), bf16),
            pltpu.VMEM((n_seqs, q_width + 2 * head_dim), f32),
            pltpu.VMEM(flat, bf16),
            pltpu.VMEM(flat, bf16),
            pltpu.VMEM((n_seqs * q_width // head_dim, head_dim), f32),
            pltpu.VMEM((n_seqs * q_width // head_dim, head_dim), f32),
            pltpu.VMEM((n_seqs, head_dim), f32),
            pltpu.VMEM((n_seqs, head_dim), f32),
            pltpu.VMEM((width // 128, 128), f32),
            pltpu.VMEM((n_seqs, head_dim), f32),
            pltpu.VMEM((n_seqs, head_dim), f32),
            pltpu.VMEM((n_seqs, width), bf16),
            dma((n_w,)),
            dma((3, n_w)),
            dma((2, n_block)),
            dma((2, n_block)),
        ],
        compiler_params=pltpu.CompilerParams(vmem_limit_bytes=55050240),
        name='layer_front',
    )(positions, resid_in, pltpu.with_memory_space_constraint(gain_attn.reshape(width // 128, 128), pltpu.HBM),
      pltpu.with_memory_space_constraint(positions[None, :], pltpu.HBM),
      rope_freqs(head_dim), w_query, w_key, w_value,
      k_cache.reshape(flat), v_cache.reshape(flat))
    return attn_out, k_out.reshape(k_cache.shape), v_out.reshape(v_cache.shape)


N_CHUNK = 16
N_SLOT = 11
T_ROWS = 1024
MESH = pl.DeviceIdType.MESH


def tail_kernel(attn_ref, resid_hbm, gain_ref, w_out_hbm, gate_t_hbm, up_t_hbm, w_down_hbm, out_ref,
                part, from_core, from_1, from_2, gathered, mid, sq_sum, resid_own, gain_f,
                gate_acc, up_acc, gate_acc_t, up_acc_t, turned, hidden, ring,
                resid_sem, out_sem, ring_sem, rs_send, rs_recv, ag_send, ag_recv):
    n_chunk, chunk = N_CHUNK, part.shape[-1]
    half = chunk // 2
    rows = mid.shape[1]
    me = lax.axis_index('tp')
    k = me % 2
    x = (me // 2) % 2
    y = me // 4
    nk, nx, ny = 1 - k, 1 - x, 1 - y
    core_nbr = {'tp': me + 1 - 2 * k}
    x_nbr = {'tp': me + 2 - 4 * x}
    y_nbr = {'tp': me + 4 - 8 * y}
    far_nbr = {'tp': me + 6 - 4 * x - 8 * y}

    def cols(c):
        return pl.ds(pl.multiple_of(c * chunk, chunk), chunk)

    depth_out = w_out_hbm.shape[0]
    first_mlp = n_chunk // 2
    first_down = first_mlp + 2 * n_chunk

    def out_slot(c):
        return c // 2, pl.ds(pl.multiple_of((c % 2) * depth_out, depth_out), depth_out)

    def out_copy(c):
        slot, span = out_slot(c)
        return pltpu.make_async_copy(w_out_hbm.at[:, cols(c)], ring.at[slot, span], out_sem.at[c % OUT_AHEAD])

    def ring_copy(src, c, j):
        slot = j % N_SLOT
        return pltpu.make_async_copy(src.at[:, cols(c)], ring.at[slot], ring_sem.at[slot])

    def gate_copy(c):
        return ring_copy(gate_t_hbm, c, first_mlp + 2 * c)

    def up_copy(c):
        return ring_copy(up_t_hbm, c, first_mlp + 2 * c + 1)

    def down_copy(c):
        return ring_copy(w_down_hbm, c, first_down + c)

    def start_load(j):
        m = j - first_mlp

        @pl.when(j < first_down)
        def _():
            @pl.when(m % 2 == 0)
            def _():
                gate_copy(m // 2).start()

            @pl.when(m % 2 == 1)
            def _():
                up_copy(m // 2).start()

        @pl.when(jnp.logical_and(j >= first_down, j < first_down + n_chunk))
        def _():
            down_copy(j - first_down).start()

    row0 = pl.multiple_of(64 * k + 32 * x + 16 * y, 16)
    resid_copy = pltpu.make_async_copy(resid_hbm.at[pl.ds(row0, rows)], resid_own, resid_sem)
    out_copy(0).start()

    barrier = pltpu.get_barrier_semaphore()
    for nbr in (core_nbr, x_nbr, y_nbr, far_nbr):
        pl.semaphore_signal(barrier, inc=1, device_id=nbr, device_id_type=MESH)

    def remote(src, dst, sems, ch, c, nbr):
        return pltpu.make_async_remote_copy(src_ref=src, dst_ref=dst, send_sem=sems[0].at[c],
                                            recv_sem=sems[1].at[ch, c], device_id=nbr, device_id_type=MESH)

    def wait_bytes(ref, sem):
        pltpu.make_async_copy(ref, ref, sem).wait()

    def wait_sent(sems, c):
        wait_bytes(mid.at[pl.ds(0, 7)], sems[0].at[c])

    rs = (rs_send, rs_recv)
    ag = (ag_send, ag_recv)
    left, right = pl.ds(0, half), pl.ds(half, half)

    def rs_core(c):
        return remote(part.at[c, nk], from_core.at[c], rs, 0, c, core_nbr)

    def rs_x1(c):
        return remote(part.at[c, k, nx, :, :, left], from_1.at[c, 0], rs, 1, c, x_nbr)

    def rs_y1(c):
        return remote(part.at[c, k, :, ny, :, right], from_1.at[c, 1], rs, 1, c, y_nbr)

    def rs_y2(c):
        return remote(part.at[c, k, x, ny, :, left], from_2.at[c, 0], rs, 2, c, y_nbr)

    def rs_x2(c):
        return remote(part.at[c, k, nx, y, :, right], from_2.at[c, 1], rs, 2, c, x_nbr)

    def ag_x(c):
        blk = gathered.at[c, k, x, y]
        return remote(blk, blk, ag, 0, c, x_nbr)

    def ag_y(c):
        blk = gathered.at[c, k, x, y]
        return remote(blk, blk, ag, 0, c, y_nbr)

    def ag_far(c):
        blk = gathered.at[c, k, x, y]
        return remote(blk, blk, ag, 1, c, far_nbr)

    def ag_fwd_y(c):
        blk = gathered.at[c, k, nx, y, :, right]
        return remote(blk, blk, ag, 1, c, y_nbr)

    def ag_fwd_x(c):
        blk = gathered.at[c, k, x, ny, :, left]
        return remote(blk, blk, ag, 1, c, x_nbr)

    def ag_core(c):
        blk = gathered.at[c, k]
        return remote(blk, blk, ag, 2, c, core_nbr)

    def stage(s, lag, fn):
        c = s - lag

        @pl.when(jnp.logical_and(c >= 0, c < n_chunk))
        def _():
            fn(c)

    def rs_stage1(c):
        rs_core(c).wait_recv()
        part[c, k] = part[c, k] + from_core[c]
        rs_x1(c).start()
        rs_y1(c).start()

    def rs_stage2(c):
        wait_bytes(from_1.at[c], rs_recv.at[1, c])
        part[c, k, x, :, :, left] = part[c, k, x, :, :, left] + from_1[c, 0]
        part[c, k, :, y, :, right] = part[c, k, :, y, :, right] + from_1[c, 1]
        rs_y2(c).start()
        rs_x2(c).start()

    def rs_stage3(c):
        wait_bytes(from_2.at[c], rs_recv.at[2, c])
        total = jnp.concatenate([part[c, k, x, y, :, left] + from_2[c, 0],
                                 part[c, k, x, y, :, right] + from_2[c, 1]], axis=-1)
        wait_sent(rs, c)
        return total

    def ag_stage1(c):
        wait_bytes(from_1.at[c], ag_recv.at[0, c])
        ag_fwd_y(c).start()
        ag_fwd_x(c).start()

    def ag_stage2(c):
        wait_bytes(from_2.at[c], ag_recv.at[1, c])
        ag_core(c).start()

    def ag_stage3(c):
        ag_core(c).wait_recv()
        block = gathered[c].reshape(8 * rows, chunk)
        wait_sent(ag, c)
        return block

    gain_f[...] = gain_ref[...].astype(jnp.float32)
    sq_sum[...] = jnp.zeros_like(sq_sum)
    gate_acc[...] = jnp.zeros_like(gate_acc)
    up_acc[...] = jnp.zeros_like(up_acc)
    gate_acc_t[...] = jnp.zeros_like(gate_acc_t)
    up_acc_t[...] = jnp.zeros_like(up_acc_t)
    for c in range(1, OUT_AHEAD):
        out_copy(c).start()
    resid_copy.start()
    pl.semaphore_wait(barrier, 4)

    def proj(c):
        out_copy(c).wait()
        slot, span = out_slot(c)
        res = jnp.dot(attn_ref[...], ring[slot, span], preferred_element_type=jnp.float32)
        part[c] = res.reshape(part.shape[1:])
        rs_core(c).start()

        @pl.when(c + OUT_AHEAD < n_chunk)
        def _():
            out_copy(c + OUT_AHEAD).start()

        ahead = first_mlp + c - LOAD_LAG

        @pl.when(jnp.logical_and(c >= LOAD_LAG, ahead < N_SLOT))
        def _():
            start_load(ahead)

        @pl.when(c % 2 == 1)
        def _():
            start_load(c // 2 + N_SLOT)

    def finish_mid(c):
        @pl.when(c == 0)
        def _():
            resid_copy.wait()

        total = rs_stage3(c)
        x1 = (resid_own[:, cols(c)].astype(jnp.float32) + total).astype(jnp.bfloat16).astype(jnp.float32)
        mid[c] = x1
        sq_sum[...] += x1 * x1

    def rs_body(s, carry):
        stage(s, 0, proj)
        stage(s, RS1_LAG[0], rs_stage1)
        stage(s, RS1_LAG[1], rs_stage2)
        stage(s, RS1_LAG[2], finish_mid)
        return carry

    lax.fori_loop(0, n_chunk + RS1_LAG[2], rs_body, 0)

    mean_sq = jnp.sum(sq_sum[...], axis=-1, keepdims=True) * (1.0 / (n_chunk * chunk))
    scale = lax.rsqrt(mean_sq + EPS)

    def send_normed(c):
        gain = jnp.concatenate([gain_f[pl.ds(c * (chunk // 128) + j, 1), :] for j in range(chunk // 128)], axis=-1)
        normed = (mid[c] * scale * gain).astype(jnp.bfloat16)
        gathered[c, k, x, y] = normed.astype(jnp.float32)
        ag_x(c).start()
        ag_y(c).start()

    def gate_up(c):
        block = ag_stage3(c).astype(jnp.bfloat16)
        gate_copy(c).wait()
        up_copy(c).wait()
        first = first_mlp + 2 * c
        accs = ((gate_acc, gate_acc_t), (up_acc, up_acc_t))
        for i, (acc, acc_t) in enumerate(accs):
            slot = (first + i) % N_SLOT
            turned[i] = ring[slot, pl.ds(T_ROWS, acc_t.shape[1])].T
            acc[...] += lax.dot_general(ring[slot, pl.ds(0, T_ROWS)], block, (((1,), (1,)), ((), ())),
                                        preferred_element_type=jnp.float32)
        for i, (acc, acc_t) in enumerate(accs):
            acc_t[...] += jnp.dot(block, turned[i], preferred_element_type=jnp.float32)
        for i in range(2):
            start_load(first + i + N_SLOT)

    def ag_body(s, carry):
        stage(s, 0, send_normed)
        stage(s, AG1_LAG[0], ag_stage1)
        stage(s, AG1_LAG[1], ag_stage2)
        stage(s, AG1_LAG[2], gate_up)
        return carry

    lax.fori_loop(0, n_chunk + AG1_LAG[2], ag_body, 0)

    def act(gate, up):
        gate = gate.astype(jnp.bfloat16).astype(jnp.float32)
        up = up.astype(jnp.bfloat16).astype(jnp.float32)
        return jax.nn.silu(gate) * up

    for lo in range(0, T_ROWS, 128):
        span = slice(lo, lo + 128)
        hidden[:, span] = act(gate_acc[span, :], up_acc[span, :]).T.astype(jnp.bfloat16)
    hidden[:, T_ROWS:] = act(gate_acc_t[...], up_acc_t[...]).astype(jnp.bfloat16)

    def down(c):
        down_copy(c).wait()
        j = first_down + c
        res = jnp.dot(hidden[...], ring[j % N_SLOT], preferred_element_type=jnp.float32)
        part[c] = res.reshape(part.shape[1:])
        rs_core(c).start()
        start_load(j + N_SLOT)

    def finish_out(c):
        total = rs_stage3(c)
        gathered[c, k, x, y] = (mid[c] + total).astype(jnp.bfloat16).astype(jnp.float32)
        ag_x(c).start()
        ag_y(c).start()

        @pl.when(c == n_chunk - 1)
        def _():
            ag_far(c).start()

    def ag_stage1_out(c):
        wait_bytes(from_1.at[c], ag_recv.at[0, c])

        @pl.when(c < n_chunk - 1)
        def _():
            ag_fwd_y(c).start()
            ag_fwd_x(c).start()

    def store_out(c):
        out_ref[:, cols(c)] = ag_stage3(c).astype(jnp.bfloat16)

    base = RS2_LAG[2]

    def down_body(s, carry):
        stage(s, 0, down)
        stage(s, RS2_LAG[0], rs_stage1)
        stage(s, RS2_LAG[1], rs_stage2)
        stage(s, base, finish_out)
        stage(s, base + AG2_LAG[0], ag_stage1_out)
        stage(s, base + AG2_LAG[1], ag_stage2)
        stage(s, base + AG2_LAG[2], store_out)
        return carry

    lax.fori_loop(0, n_chunk + base + AG2_LAG[2], down_body, 0)


RS1_LAG = (2, 6, 10)
AG1_LAG = (2, 4, 5)
RS2_LAG = (2, 5, 8)
AG2_LAG = (2, 4, 5)
OUT_AHEAD = 4
LOAD_LAG = 4


def layer_tail(attn_out, resid_in, gain_mlp, w_out, w_gate, w_up, w_down):
    n_rows, width = resid_in.shape
    ffn = w_gate.shape[1]
    chunk = width // N_CHUNK
    half = chunk // 2
    rows = n_rows // 8
    f32, bf16 = jnp.float32, jnp.bfloat16
    vmem = pl.BlockSpec(memory_space=pltpu.VMEM)
    hbm = pl.BlockSpec(memory_space=pl.ANY)
    dma = pltpu.SemaphoreType.DMA
    return pl.pallas_call(
        tail_kernel,
        out_shape=jax.ShapeDtypeStruct((n_rows, width), bf16),
        in_specs=[vmem, hbm, vmem, hbm, hbm, hbm, hbm],
        out_specs=vmem,
        scratch_shapes=[
            pltpu.VMEM((N_CHUNK, 2, 2, 2, rows, chunk), f32),
            pltpu.VMEM((N_CHUNK, 2, 2, rows, chunk), f32),
            pltpu.VMEM((N_CHUNK, 2, 2, rows, half), f32),
            pltpu.VMEM((N_CHUNK, 2, rows, half), f32),
            pltpu.VMEM((N_CHUNK, 2, 2, 2, rows, chunk), f32),
            pltpu.VMEM((N_CHUNK, rows, chunk), f32),
            pltpu.VMEM((rows, chunk), f32),
            pltpu.VMEM((rows, width), bf16),
            pltpu.VMEM((width // 128, 128), f32),
            pltpu.VMEM((T_ROWS, n_rows), f32),
            pltpu.VMEM((T_ROWS, n_rows), f32),
            pltpu.VMEM((n_rows, ffn - T_ROWS), f32),
            pltpu.VMEM((n_rows, ffn - T_ROWS), f32),
            pltpu.VMEM((2, chunk, ffn - T_ROWS), bf16),
            pltpu.VMEM((n_rows, ffn), bf16),
            pltpu.VMEM((N_SLOT, ffn, chunk), bf16),
            dma(()),
            dma((OUT_AHEAD,)),
            dma((N_SLOT,)),
            dma((N_CHUNK,)),
            dma((3, N_CHUNK)),
            dma((N_CHUNK,)),
            dma((3, N_CHUNK)),
        ],
        compiler_params=pltpu.CompilerParams(collective_id=0, has_side_effects=True,
                                             vmem_limit_bytes=53477376),
        name='layer_tail',
    )(attn_out, resid_in, gain_mlp.reshape(width // 128, 128), w_out, w_gate.T, w_up.T, w_down)


def solution(mesh):
    def layer_local(resid_in, positions, k_cache, v_cache, gain_attn, w_query, w_key, w_value,
                    w_out, gain_mlp, w_gate, w_up, w_down):
        attn_out, k_full, v_full = layer_front(resid_in, positions, k_cache, v_cache,
                                               gain_attn, w_query, w_key, w_value)
        resid_out = layer_tail(attn_out, resid_in, gain_mlp, w_out, w_gate, w_up, w_down)
        return resid_out, k_full, v_full

    row_spec = P('dp', None)
    cache_spec = P('dp', None, 'tp', None)
    col_spec = P(None, 'tp')
    split_rows = P('tp', None)
    return jax.shard_map(layer_local, mesh=mesh,
                         in_specs=(row_spec, P('dp'), cache_spec, cache_spec, P(), col_spec, col_spec,
                                   col_spec, split_rows, P(), col_spec, col_spec, split_rows),
                         out_specs=(row_spec, cache_spec, cache_spec), check_vma=False)
```
